32 devices in a mesh: gx: 4 (over z), gy: 4 (over y, x), gz: 2 (over core).
Axes of the slice: x: 2, y: 2, z: 4, core: 2. Of those that a mesh axis runs over, the one named last changes fastest.
Arguments:
- cell_index: int32 [4, 4, 2, 8192], P('gx', 'gy', 'gz'), may hold values from 1431 to 167568, as said below
- offsets: float32 [4, 4, 2, 3, 8192], P('gx', 'gy', 'gz'), may hold values from -0.5 to 0.5
- mass: float32 [4, 4, 2, 8192], P('gx', 'gy', 'gz'), may hold values from 0.5 to 2
- counts: int32 [4, 4, 2], P('gx', 'gy', 'gz'), may hold values from 2048 to 8192, as said below
Outputs:
- density: float32 [512, 4, 8, 256], P(None, 'gx', 'gy', 'gz')
- spectrum: float32 [2, 256, 4, 8, 256], P(None, None, 'gx', 'gy', 'gz')
The draws below stay inside these ranges and needn't reach their ends.
Inputs may be any that keep to these rules, and one draw needn't show every extreme that they name: `cell_index`: each entry is (i + 1) * 10 * 130 + (j + 1) * 130 + k + 1 for a cell (i, j, k) with 0 <= i < 128, 0 <= j < 8, 0 <= k < 128; slots past a block's count hold such indices too. `counts`: some block is full in every draw.
All inputs are finite; a program needn't handle non-finite values.
Results may differ from the reference program's by a relative error of at most 0.0003.
Values sent between devices are 32-bit elements; how exact they have to be, the bound alone decides.
A program may use at most 64 MiB of HBM per device.

```python
import math
import jax
import jax.numpy as jnp
from jax import lax

CX = 128
YP = 2
CZ = 128
PCAP = 8192
CY = 8
NX = 512
NY = 32
NZ = 256
N_GX = 4
N_GY = 4
N_GZ = 2


def edge_biased(key, extent, full_shape):
    pick_key, place_key = jax.random.split(key)
    selector = jax.random.randint(pick_key, full_shape, 0, 8)
    spread = jax.random.randint(place_key, full_shape, 0, extent)
    return jnp.where(selector == 0, 0, jnp.where(selector == 1, extent - 1, spread)).astype(jnp.int32)


def draw_cell_index(key, part):
    full_shape = (N_GX, N_GY, N_GZ, PCAP)
    key_list = jax.random.split(jax.random.fold_in(key, 11), 3)
    coord_x = edge_biased(key_list[0], CX, full_shape)
    coord_y = edge_biased(key_list[1], CY, full_shape)
    coord_z = edge_biased(key_list[2], CZ, full_shape)
    return (((coord_x + 1) * (CY + 2) + coord_y + 1) * (CZ + 2) + coord_z + 1).astype(jnp.int32)


def draw_counts(key, part):
    full_shape = (N_GX, N_GY, N_GZ)
    key_list = jax.random.split(jax.random.fold_in(key, 23), 3)
    base_load = jax.random.randint(key_list[0], full_shape, PCAP // 4, PCAP // 2 + 1)
    heavy = jax.random.randint(key_list[1], full_shape, 0, 16) == 0
    loads = jnp.where(heavy, PCAP, base_load).reshape(-1)
    fullest = jax.random.randint(key_list[2], (), 0, N_GX * N_GY * N_GZ)
    loads = loads.at[fullest].set(PCAP)
    return loads.reshape(full_shape).astype(jnp.int32)


def shard_levels(rng, dims, shards, low, high):
    def one(axis_at, parts):
        steps = jax.random.uniform(jax.random.fold_in(jax.random.fold_in(rng, 6), axis_at), (parts,), jnp.float32, low / len(shards), high / len(shards))
        return jnp.repeat(jnp.exp(steps), dims[axis_at] // parts).reshape((-1,) + (1,) * (len(dims) - axis_at - 1))

    loudness = one(*shards[0])
    for cut in shards[1:]:
        loudness = loudness * one(*cut)
    return loudness


def setup_inputs(seed: int = 0) -> dict:
    keys = jax.random.split(jax.random.key(seed), 5)
    cell_index = draw_cell_index(jax.random.fold_in(keys[4], 71), 0)
    offsets = jnp.clip(jax.random.uniform(keys[1], (N_GX, N_GY, N_GZ, 3, PCAP), jnp.float32, -0.5, 0.5) * shard_levels(keys[1], (N_GX, N_GY, N_GZ, 3, PCAP), ((0, 4), (1, 4), (2, 2)), -0.4, 0.0), -0.5, 0.5)
    mass = jnp.clip(jnp.exp(math.log(2.0) - 1.3862944 * jax.random.uniform(keys[2], (N_GX, N_GY, N_GZ, PCAP), jnp.float32) ** shard_levels(keys[2], (N_GX, N_GY, N_GZ, PCAP), ((0, 4), (1, 4), (2, 2)), -0.2, 0.2)), 0.5, 2.0)
    counts = draw_counts(jax.random.fold_in(keys[4], 71), 0)
    return {"cell_index": cell_index, "offsets": offsets, "mass": mass, "counts": counts}


def to_pencils(field):
    leading = field.shape[:-3]
    split = field.reshape(leading + (field.shape[-3], N_GY, N_GX, YP, NZ))
    moved = jnp.moveaxis(split, -4, -3)
    return moved.reshape(leading + (field.shape[-3], N_GX, N_GY * YP, NZ))

def reference(cell_index, offsets, mass, counts):
    full_shape = (N_GX, N_GY, N_GZ, PCAP)
    plane = (CY + 2) * (CZ + 2)
    block_x = lax.broadcasted_iota(jnp.int32, full_shape, 0)
    block_y = lax.broadcasted_iota(jnp.int32, full_shape, 1)
    block_z = lax.broadcasted_iota(jnp.int32, full_shape, 2)
    slot_ids = lax.broadcasted_iota(jnp.int32, full_shape, 3)
    pos_x = cell_index // plane - 1 + block_x * CX
    pos_y = cell_index // (CZ + 2) % (CY + 2) - 1 + block_y * CY
    pos_z = cell_index % (CZ + 2) - 1 + block_z * CZ
    loaded = jnp.where(slot_ids < counts[..., None], mass, jnp.float32(0.0))
    positions = (pos_x, pos_y, pos_z)
    extents = (NX, NY, NZ)
    shifts = [offsets[:, :, :, axis_pos, :] for axis_pos in range(3)]
    signs = [jnp.where(shifts[axis_pos] >= 0.0, 1, -1).astype(jnp.int32) for axis_pos in range(3)]
    field = jnp.zeros((NX * NY * NZ,), jnp.float32)
    for corner in range(8):
        factor = None
        targets = []
        for axis_pos in range(3):
            upper_bit = corner >> 2 - axis_pos & 1
            magnitude = jnp.abs(shifts[axis_pos])
            if upper_bit:
                target = (positions[axis_pos] + signs[axis_pos]) % extents[axis_pos]
                factor_one = magnitude
            else:
                target = positions[axis_pos] % extents[axis_pos]
                factor_one = 1.0 - magnitude
            targets.append(target.astype(jnp.int32))
            factor = factor_one if factor is None else factor * factor_one
        weight = factor * loaded
        flat_cell = ((targets[0] * NY + targets[1]) * NZ + targets[2]).astype(jnp.int32)
        field = field.at[flat_cell.reshape(-1)].add(weight.reshape(-1))
    field = field.reshape(NX, NY, NZ)
    modes = jnp.fft.rfft(field, axis=0)[:NX // 2]
    scale = 1.0 / math.sqrt(NX)
    spectrum = jnp.stack([jnp.real(modes), jnp.imag(modes)]).astype(jnp.float32) * scale
    return (to_pencils(field), to_pencils(spectrum))
```

```python
import functools
import math

import jax
import jax.numpy as jnp
import numpy as np
from jax import lax
from jax.experimental import pallas as pl
from jax.experimental.pallas import tpu as pltpu
from jax.sharding import PartitionSpec as P

MESH = pl.DeviceIdType.MESH
CX = 128
YP = 2
CZ = 128


def up(n, m):
    return -(-n // m) * m


def split(value):
    high = value.astype(jnp.bfloat16)
    low = (value - high.astype(jnp.float32)).astype(jnp.bfloat16)
    return high, low


def nt_dot(lhs, rhs):
    return lax.dot_general(lhs, rhs, (((1,), (1,)), ((), ())), preferred_element_type=jnp.float32)


def gather(full, rows):
    return (full[:rows, :128] + full[rows:, :128]) + (full[:rows, 128:] + full[rows:, 128:])


BODY = YP * CX
ROWS = BODY + 8


def parts(value):
    high = value.astype(jnp.bfloat16).astype(jnp.float32)
    return high, value - high


def paint_kernel(dims, live_ref, cell_ref, off_ref, mass_ref, out_ref, rows_x, rows_z, weigh, spot, zrhs, xrhs, lhs, glhs, crhs, accx, accz, accc, columns, fold_x, fold_z, zin, yout, yin, pen, inbox, z_send, z_recv, y_send, y_recv, x_send, x_recv):
    groups, count_y, count_z = dims
    padded_y = YP * groups + 2
    band = up(padded_y, 16)
    stride_y = CZ + 2
    stride_x = padded_y * stride_y
    lines = cell_ref.shape[0]
    span = min(16, lines)
    pieces = lines // span
    gx, gy, gz = lax.axis_index("gx"), lax.axis_index("gy"), lax.axis_index("gz")
    y_next = (lax.rem(gy + count_y - 1, count_y), lax.rem(gy + 1, count_y))
    z_next = (lax.rem(gz + count_z - 1, count_z), lax.rem(gz + 1, count_z))
    barrier = pltpu.get_barrier_semaphore()
    for other in z_next:
        pl.semaphore_signal(barrier, inc=1, device_id={"gz": other}, device_id_type=MESH)
    for other in y_next:
        pl.semaphore_signal(barrier, inc=1, device_id={"gy": other}, device_id_type=MESH)
    for step in range(1, groups):
        pl.semaphore_signal(barrier, inc=1, device_id={"gx": lax.rem(gx + step, groups)}, device_id_type=MESH)

    live = live_ref[0]
    slot = lax.broadcasted_iota(jnp.int32, (lines, 128), 0) * 128 + lax.broadcasted_iota(jnp.int32, (lines, 128), 1)
    loaded = jnp.where(slot < live, mass_ref[...], 0.0)
    cell = cell_ref[...].astype(jnp.float32)
    x0 = jnp.floor((cell + 0.5) * (1.0 / stride_x))
    rest = cell - x0 * stride_x
    y0 = jnp.floor((rest + 0.5) * (1.0 / stride_y))
    z0 = rest - y0 * stride_y
    dx, dy, dz = off_ref[0], off_ref[1], off_ref[2]
    x1 = x0 + jnp.where(dx >= 0.0, 1.0, -1.0)
    y1 = y0 + jnp.where(dy >= 0.0, 1.0, -1.0)
    z1 = z0 + jnp.where(dz >= 0.0, 1.0, -1.0)
    fx, fy, fz = jnp.abs(dx), jnp.abs(dy), jnp.abs(dz)
    ex, ey, ez = 1.0 - fx, 1.0 - fy, 1.0 - fz
    my0, my1 = ey * loaded, fy * loaded
    spot[0], spot[1], spot[2], spot[3] = y0, y1, my0, my1
    spot[4], spot[5] = ex, fx
    for index, value in enumerate((x0, x1) + parts(ex) + parts(fx)):
        rows_x[index] = value
    for index, value in enumerate((z0, z1) + parts(ez) + parts(fz)):
        rows_z[index] = value
    far_x, far_z = CX + 1.0, CZ + 1.0
    gx_y = jnp.where(x1 == 0.0, 0.0, jnp.where(x1 == far_x, float(band), -1.0 - band))
    gz_y = jnp.where(z1 == 0.0, 0.0, jnp.where(z1 == far_z, float(band), -1.0 - band))
    ghost_rows = (
        (gz_y + y0, gz_y + y1) + parts(fz * my0) + parts(fz * my1),
        (gx_y + y0, gx_y + y1) + parts(fx * my0) + parts(fx * my1),
    )
    for kind in range(2):
        for index, value in enumerate(ghost_rows[kind]):
            weigh[8 + 6 * kind + index] = value

    def row(ref, index, line):
        value = ref[index, pl.ds(line, 1), :]
        return jnp.broadcast_to(value, (16, 128)).astype(jnp.bfloat16)[None]

    zero = jnp.zeros((1, 16, 128), jnp.bfloat16)
    count = lax.broadcasted_iota(jnp.int32, (CX // 16, 16, 128), 0) * 16 + lax.broadcasted_iota(jnp.int32, (CX // 16, 16, 128), 1)
    core = (count + 1).astype(jnp.float32).astype(jnp.bfloat16)
    banded = count.astype(jnp.float32).astype(jnp.bfloat16)[: 2 * band // 16]
    sides = lax.broadcasted_iota(jnp.int32, (1, 16, 128), 1)
    side_row = jnp.where(lax.rem(sides, 2) == 0, 0.0, far_x).astype(jnp.bfloat16)
    top = jnp.where(sides < 2, 1.0, 0.0).astype(jnp.bfloat16)

    def hot(ref, line, at=0, rows=core):
        first, second = rows == row(ref, at, line), rows == row(ref, at + 1, line)
        high = jnp.where(first, row(ref, at + 2, line), jnp.where(second, row(ref, at + 4, line), zero))
        low = jnp.where(first, row(ref, at + 3, line), jnp.where(second, row(ref, at + 5, line), zero))
        return high.reshape(-1, 128), low.reshape(-1, 128)

    def across(piece, store):
        for line in range(span):
            store(piece * span + line)

    def build_ghost(kind):
        def store(line):
            high, low = hot(weigh, line, 8 + 6 * kind, banded)
            glhs[kind, line, pl.ds(0, 2 * band)] = high
            glhs[kind, line, pl.ds(2 * band, 2 * band)] = low

        return store

    def build_x(line):
        high, low = hot(rows_x, line)
        xrhs[line, pl.ds(0, CX)] = high
        xrhs[line, pl.ds(CX, CX)] = low
        match = side_row == row(rows_x, 1, line)
        pick = jnp.where(top > zero, row(rows_x, 4, line), row(rows_x, 5, line))
        crhs[line] = jnp.where(match, pick, zero).reshape(16, 128)

    def build_z(line):
        high, low = hot(rows_z, line)
        zrhs[line, pl.ds(0, CZ)] = high
        zrhs[line, pl.ds(CZ, CZ)] = low

    def wide(ref, piece):
        return jnp.concatenate([ref[piece * span + line] for line in range(span)], axis=1)

    def total(terms):
        sums = None
        for term in terms:
            sums = term if sums is None else sums + term
        return sums

    accx[...] = jnp.zeros_like(accx)
    accz[...] = jnp.zeros_like(accz)
    accc[...] = jnp.zeros_like(accc)

    def prepare(piece, carry):
        across(piece, build_x)
        across(piece, build_ghost(0))
        across(piece, build_z)
        across(piece, build_ghost(1))
        accz[...] += nt_dot(wide(glhs.at[0], piece), wide(xrhs, piece))
        accx[...] += nt_dot(wide(glhs.at[1], piece), wide(zrhs, piece))
        accc[...] += nt_dot(wide(glhs.at[0], piece), wide(crhs, piece))
        return carry

    lax.fori_loop(0, pieces, prepare, 0)
    fold_z[:, :CX] = gather(accz[...], 2 * band)
    ends = accc[pl.ds(0, 2 * band)] + accc[pl.ds(2 * band, 2 * band)]
    fold_z[:, CX:] = jnp.zeros((2 * band, CX), jnp.float32)
    fold_z[:, CX : CX + 2] = ends[:, :2] + ends[:, 2:4]
    z_copies = [
        pltpu.make_async_remote_copy(
            src_ref=fold_z.at[pl.ds(side * band, band)],
            dst_ref=zin.at[side],
            send_sem=z_send.at[side],
            recv_sem=z_recv.at[side],
            device_id={"gz": z_next[side]},
            device_id_type=MESH,
        )
        for side in range(2)
    ]

    def paint_rows(first, second):
        for index, y in enumerate((first, second)):
            wy = jnp.where(spot[0] == y, spot[2], jnp.where(spot[1] == y, spot[3], 0.0))
            for place, value in enumerate(parts(spot[4] * wy) + parts(spot[5] * wy)):
                weigh[4 * index + place] = value

        def build(line):
            near, far = core == row(rows_x, 0, line), core == row(rows_x, 1, line)
            for index in range(2):
                for part in range(2):
                    value = jnp.where(near, row(weigh, 4 * index + part, line), jnp.where(far, row(weigh, 4 * index + 2 + part, line), zero))
                    lhs[line, pl.ds((2 * index + part) * CX, CX)] = value.reshape(CX, 128)

        terms = []
        for piece in range(pieces):
            across(piece, build)
            terms.append(nt_dot(wide(lhs, piece), wide(zrhs, piece)))
        sums = total(terms)
        return gather(sums[: 2 * CX], CX), gather(sums[2 * CX :], CX)

    lane = lax.broadcasted_iota(jnp.int32, (CX, CZ), 1)
    band_row = lax.broadcasted_iota(jnp.int32, (2 * CX, band), 1)
    half = groups // 2
    upper = gx // half

    def pencil_of(turn):
        mine = upper * (groups - 1) + (1 - 2 * upper) * gx
        near_by = turn - (groups - half)
        near_by = near_by + jnp.where(near_by >= mine, 1, 0)
        place = jnp.where(turn < groups - half, half + turn, jnp.where(turn == groups - 1, mine, near_by))
        return upper * (groups - 1) + (1 - 2 * upper) * place

    def part_copy(target, part):
        size = CX if part is not YP else 8
        here = pl.ds(pl.multiple_of(part * CX, 8), size)
        return pltpu.make_async_remote_copy(
            src_ref=pen.at[target, here],
            dst_ref=inbox.at[gx, here],
            send_sem=x_send.at[part, target],
            recv_sem=x_recv.at[part, gx],
            device_id={"gx": target},
            device_id_type=MESH,
        )

    y_copies = [
        pltpu.make_async_remote_copy(
            src_ref=yout.at[pl.ds(side * CX, CX)],
            dst_ref=yin.at[side],
            send_sem=y_send.at[side],
            recv_sem=y_recv.at[side],
            device_id={"gy": y_next[side]},
            device_id_type=MESH,
        )
        for side in range(2)
    ] + [
        pltpu.make_async_remote_copy(
            src_ref=yout.at[pl.ds(BODY, 8)],
            dst_ref=yin.at[2 + side, pl.ds(0, 8)],
            send_sem=y_send.at[2 + side],
            recv_sem=y_recv.at[2 + side],
            device_id={"gy": y_next[side]},
            device_id_type=MESH,
        )
        for side in range(2)
    ]
    yout[pl.ds(BODY, 8)] = jnp.zeros((8, CZ), jnp.float32)
    for target in range(groups):
        pen[target, pl.ds(BODY, 8)] = jnp.zeros((8, CZ), jnp.float32)

    def fold_into(target, rows, indices):
        for place, (whole, index) in enumerate(zip(rows, indices)):
            for side, edge_lane in enumerate((CZ - 1, 0)):
                column = jnp.sum(jnp.where(band_row == index, columns[side], 0.0), axis=1, keepdims=True)
                whole = whole + jnp.where(lane == edge_lane, column[:CX], 0.0)
            target[pl.ds(place * CX, CX)] = whole
            for side in range(2):
                target[pl.ds(BODY + 2 * side + place, 1)] = fold_x[side, pl.ds(index, 1)]

    def add_first():
        pen[0, pl.ds(0, CX)] += yin[1]
        for side in range(2):
            pen[0, pl.ds(BODY + 2 * side, 1)] += yin[3, pl.ds(2 * side + 1, 1)]

    def add_last():
        pen[groups - 1, pl.ds((YP - 1) * CX, CX)] += yin[0]
        for side in range(2):
            pen[groups - 1, pl.ds(BODY + 2 * side + YP - 1, 1)] += yin[2, pl.ds(2 * side, 1)]

    late = groups - half

    def visit(turn, carry):
        ghost = turn == 1
        order = jnp.where(turn == 0, 0, turn - 1)
        target = pencil_of(order)
        first = jnp.where(ghost, 0, 1 + target * YP)
        second = jnp.where(ghost, padded_y - 1, 2 + target * YP)
        rows = paint_rows(first.astype(jnp.float32), second.astype(jnp.float32))

        @pl.when(turn == 0)
        def _():
            pl.semaphore_wait(barrier, groups + 3)
            for copy in z_copies:
                copy.start()
            edge = gather(accx[...], 2 * band)
            for copy in z_copies:
                copy.wait()
            edge_lane = lax.broadcasted_iota(jnp.int32, (band, CZ), 1)
            for side in range(2):
                columns[side] = zin[side].T
                part = edge[side * band : (side + 1) * band]
                part = part + jnp.where(edge_lane == CZ - 1, zin[0][:, CX + side : CX + side + 1], 0.0)
                fold_x[side] = part + jnp.where(edge_lane == 0, zin[1][:, CX + side : CX + side + 1], 0.0)

        @pl.when(ghost)
        def _():
            fold_into(yout, rows, (first, second))
            for copy in y_copies:
                copy.start()

        @pl.when(jnp.logical_not(ghost))
        def _():
            fold_into(pen.at[target], rows, (first, second))

            @pl.when(turn > late)
            def _():
                @pl.when(turn == late + 1)
                def _():
                    for copy in y_copies:
                        copy.wait()

                @pl.when(jnp.logical_or(target == 0, jnp.logical_and(turn == late + 1, upper == 1)))
                def _():
                    add_first()

                @pl.when(jnp.logical_or(target == groups - 1, jnp.logical_and(turn == late + 1, upper == 0)))
                def _():
                    add_last()

                @pl.when(turn == late + 1)
                def _():
                    held = (1 - upper) * (groups - 1)
                    part_copy(held, (1 - upper) * (YP - 1)).start()
                    part_copy(held, YP).start()

            @pl.when(turn < groups)
            def _():
                @pl.when(turn == late)
                def _():
                    part_copy(target, upper * (YP - 1)).start()

                @pl.when(turn != late)
                def _():
                    for part in range(YP + 1):
                        part_copy(target, part).start()

        return carry

    lax.fori_loop(0, groups + 1, visit, 0)
    out_ref[gx] = pen[gx]
    for step in range(1, groups):
        source = lax.rem(gx + step, groups)
        for part in range(YP + 1):
            here = pl.ds(part * CX, CX if part < YP else 8)
            part_copy(source, part).wait_send()
            pltpu.make_async_remote_copy(
                src_ref=pen.at[source, here],
                dst_ref=inbox.at[source, here],
                send_sem=x_send.at[part, source],
                recv_sem=x_recv.at[part, source],
                device_id={"gx": source},
                device_id_type=MESH,
            ).wait_recv()
        out_ref[source] = inbox[source]


def paint(dims, cell, offs, mass, live):
    groups = dims[0]
    lines = cell.shape[0]
    band = up(YP * groups + 2, 16)
    vmem = pl.BlockSpec(memory_space=pltpu.VMEM)
    dma = pltpu.SemaphoreType.DMA
    return pl.pallas_call(
        functools.partial(paint_kernel, dims),
        out_shape=jax.ShapeDtypeStruct((groups, ROWS, CZ), jnp.float32),
        in_specs=[pl.BlockSpec(memory_space=pltpu.SMEM), vmem, vmem, vmem],
        out_specs=vmem,
        scratch_shapes=[
            pltpu.VMEM((6, lines, 128), jnp.float32),
            pltpu.VMEM((6, lines, 128), jnp.float32),
            pltpu.VMEM((20, lines, 128), jnp.float32),
            pltpu.VMEM((6, lines, 128), jnp.float32),
            pltpu.VMEM((lines, 2 * CZ, 128), jnp.bfloat16),
            pltpu.VMEM((lines, 2 * CX, 128), jnp.bfloat16),
            pltpu.VMEM((lines, 2 * BODY, 128), jnp.bfloat16),
            pltpu.VMEM((2, lines, 4 * band, 128), jnp.bfloat16),
            pltpu.VMEM((lines, 16, 128), jnp.bfloat16),
            pltpu.VMEM((4 * band, 256), jnp.float32),
            pltpu.VMEM((4 * band, 256), jnp.float32),
            pltpu.VMEM((4 * band, 16), jnp.float32),
            pltpu.VMEM((2, 2 * CX, band), jnp.float32),
            pltpu.VMEM((2, band, CZ), jnp.float32),
            pltpu.VMEM((2 * band, 2 * CX), jnp.float32),
            pltpu.VMEM((2, band, 2 * CX), jnp.float32),
            pltpu.VMEM((ROWS, CZ), jnp.float32),
            pltpu.VMEM((4, CX, CZ), jnp.float32),
            pltpu.VMEM((groups, ROWS, CZ), jnp.float32),
            pltpu.VMEM((groups, ROWS, CZ), jnp.float32),
            dma((2,)),
            dma((2,)),
            dma((4,)),
            dma((4,)),
            dma((YP + 1, groups)),
            dma((YP + 1, groups)),
        ],
        compiler_params=pltpu.CompilerParams(collective_id=0, has_side_effects=True),
    )(live, cell, offs, mass)


def wave_kernel(groups, in_ref, fhi, flo, dens_ref, spec_ref, flat):
    length = groups * CX
    row_id = lax.broadcasted_iota(jnp.int32, (CX, CZ), 0)
    for block in range(groups):
        before, after = (block - 1) % groups, (block + 1) % groups
        for row in range(YP):
            value = in_ref[block, row * CX : (row + 1) * CX]
            upper = BODY + 2 + row
            value = value + jnp.where(row_id == 0, in_ref[before, upper : upper + 1], 0.0)
            lower = BODY + row
            value = value + jnp.where(row_id == CX - 1, in_ref[after, lower : lower + 1], 0.0)
            dens_ref[pl.ds(block * BODY + row, CX, stride=YP), :] = value
            high, low = split(value)
            flat[0, pl.ds(block * CX, CX), pl.ds(row * CZ, CZ)] = high
            flat[1, pl.ds(block * CX, CX), pl.ds(row * CZ, CZ)] = low
    tile = 256

    def transform(turn, carry):
        start = pl.multiple_of(turn * tile, tile)
        rows = pl.ds(start, tile)
        both = jnp.dot(fhi[rows, :], flat[0], preferred_element_type=jnp.float32)
        both += jnp.dot(flo[rows, :], flat[0], preferred_element_type=jnp.float32)
        both += jnp.dot(fhi[rows, :], flat[1], preferred_element_type=jnp.float32)
        for row in range(YP):
            spec_ref[pl.ds(start * YP + row, tile, stride=YP), :] = both[:, row * CZ : (row + 1) * CZ]
        return carry

    lax.fori_loop(0, length // tile, transform, 0)


def waves(groups, pencils):
    length = groups * CX
    half = length // 2
    angle = (np.arange(half)[:, None] * np.arange(length)[None, :] % length) * (2.0 * np.pi / length)
    table = np.concatenate([np.cos(angle), -np.sin(angle)]) / np.sqrt(length)
    fhi = table.astype(jnp.bfloat16)
    flo = (table - fhi.astype(np.float64)).astype(jnp.bfloat16)
    vmem = pl.BlockSpec(memory_space=pltpu.VMEM)
    return pl.pallas_call(
        functools.partial(wave_kernel, groups),
        out_shape=[
            jax.ShapeDtypeStruct((length * YP, CZ), jnp.float32),
            jax.ShapeDtypeStruct((2 * half * YP, CZ), jnp.float32),
        ],
        in_specs=[vmem] * 3,
        out_specs=[vmem] * 2,
        scratch_shapes=[pltpu.VMEM((2, length, YP * CZ), jnp.bfloat16)],
    )(pencils, jnp.asarray(fhi), jnp.asarray(flo))


def body(dims, cell_index, offsets, mass, counts):
    length = dims[0] * CX
    pencils = paint(
        dims, cell_index.reshape(-1, 128), offsets.reshape(3, -1, 128), mass.reshape(-1, 128), counts.reshape(1)
    )
    density, spectrum = waves(dims[0], pencils)
    return (density.reshape(length, 1, YP, CZ), spectrum.reshape(2, length // 2, 1, YP, CZ))


def solution(mesh):
    dims = tuple(mesh.shape[axis] for axis in ("gx", "gy", "gz"))
    placed = (
        P("gx", "gy", "gz", None),
        P("gx", "gy", "gz", None, None),
        P("gx", "gy", "gz", None),
        P("gx", "gy", "gz"),
    )
    return jax.shard_map(
        functools.partial(body, dims),
        mesh=mesh,
        in_specs=placed,
        out_specs=(P(None, "gx", "gy", "gz"), P(None, None, "gx", "gy", "gz")),
        check_vma=False,
    )
```

```python
import functools
import math

import jax
import jax.numpy as jnp
import numpy as np
from jax import lax
from jax.experimental import pallas as pl
from jax.experimental.pallas import tpu as pltpu
from jax.sharding import PartitionSpec as P

MESH = pl.DeviceIdType.MESH
CX = 128
YP = 2
CZ = 128


def up(n, m):
    return -(-n // m) * m


def split(value):
    high = value.astype(jnp.bfloat16)
    low = (value - high.astype(jnp.float32)).astype(jnp.bfloat16)
    return high, low


def nt_dot(lhs, rhs):
    return lax.dot_general(lhs, rhs, (((1,), (1,)), ((), ())), preferred_element_type=jnp.float32)


def gather(full, rows):
    return (full[:rows, :128] + full[rows:, :128]) + (full[:rows, 128:] + full[rows:, 128:])


BODY = YP * CX
ROWS = BODY + 8


def parts(value):
    high = value.astype(jnp.bfloat16).astype(jnp.float32)
    return high, value - high


def paint_kernel(dims, live_ref, cell_hbm, off_hbm, mass_hbm, out_ref, cell_ref, off_ref, mass_ref, rows_x, rows_z, weigh, spot, zrhs, xrhs, lhs, glhs, crhs, accz, accc, columns, corner, fold_z, zin, yout, yin, pen, load, z_send, z_recv, y_send, y_recv, x_send, x_recv):
    groups, count_y, count_z = dims
    padded_y = YP * groups + 2
    band = up(padded_y, 16)
    loads = [
        pltpu.make_async_copy(source, target, load.at[index])
        for index, (source, target) in enumerate(((cell_hbm, cell_ref), (off_hbm, off_ref), (mass_hbm, mass_ref)))
    ]
    for copy in loads:
        copy.start()
    stride_y = CZ + 2
    stride_x = padded_y * stride_y
    lines = cell_ref.shape[0]
    span = min(16, lines)
    pieces = lines // span
    gx, gy, gz = lax.axis_index("gx"), lax.axis_index("gy"), lax.axis_index("gz")
    y_next = (lax.rem(gy + count_y - 1, count_y), lax.rem(gy + 1, count_y))
    z_next = (lax.rem(gz + count_z - 1, count_z), lax.rem(gz + 1, count_z))
    barrier = pltpu.get_barrier_semaphore()
    for other in z_next:
        pl.semaphore_signal(barrier, inc=1, device_id={"gz": other}, device_id_type=MESH)
    for other in y_next:
        pl.semaphore_signal(barrier, inc=1, device_id={"gy": other}, device_id_type=MESH)
    for step in range(1, groups):
        pl.semaphore_signal(barrier, inc=1, device_id={"gx": lax.rem(gx + step, groups)}, device_id_type=MESH)

    for copy in loads:
        copy.wait()
    live = live_ref[0]
    slot = lax.broadcasted_iota(jnp.int32, (lines, 128), 0) * 128 + lax.broadcasted_iota(jnp.int32, (lines, 128), 1)
    loaded = jnp.where(slot < live, mass_ref[...], 0.0)
    cell = cell_ref[...].astype(jnp.float32)
    x0 = jnp.floor((cell + 0.5) * (1.0 / stride_x))
    rest = cell - x0 * stride_x
    y0 = jnp.floor((rest + 0.5) * (1.0 / stride_y))
    z0 = rest - y0 * stride_y
    dx, dy, dz = off_ref[0], off_ref[1], off_ref[2]
    x1 = x0 + jnp.where(dx >= 0.0, 1.0, -1.0)
    y1 = y0 + jnp.where(dy >= 0.0, 1.0, -1.0)
    z1 = z0 + jnp.where(dz >= 0.0, 1.0, -1.0)
    fx, fy, fz = jnp.abs(dx), jnp.abs(dy), jnp.abs(dz)
    ex, ey, ez = 1.0 - fx, 1.0 - fy, 1.0 - fz
    my0, my1 = ey * loaded, fy * loaded
    spot[0], spot[1], spot[2], spot[3] = y0, y1, my0, my1
    spot[4], spot[5] = ex, fx
    for index, value in enumerate((x0, x1) + parts(ex) + parts(fx)):
        rows_x[index] = value
    for index, value in enumerate((z0, z1) + parts(ez) + parts(fz)):
        rows_z[index] = value
    far_x, far_z = CX + 1.0, CZ + 1.0
    gz_y = jnp.where(z1 == 0.0, 0.0, jnp.where(z1 == far_z, float(band), -1.0 - band))
    ghost_rows = (gz_y + y0, gz_y + y1) + parts(fz * my0) + parts(fz * my1)
    for index, value in enumerate(ghost_rows):
        weigh[8 + index] = value

    def row(ref, index, line):
        value = ref[index, pl.ds(line, 1), :]
        return jnp.broadcast_to(value, (16, 128)).astype(jnp.bfloat16)[None]

    zero = jnp.zeros((1, 16, 128), jnp.bfloat16)
    count = lax.broadcasted_iota(jnp.int32, (CX // 16, 16, 128), 0) * 16 + lax.broadcasted_iota(jnp.int32, (CX // 16, 16, 128), 1)
    core = (count + 1).astype(jnp.float32).astype(jnp.bfloat16)
    banded = count.astype(jnp.float32).astype(jnp.bfloat16)[: 2 * band // 16]
    sides = lax.broadcasted_iota(jnp.int32, (1, 16, 128), 1)
    edge_row = jnp.where(sides < 4 * YP, jnp.where(lax.rem(sides, 2) == 0, 0.0, far_x), -9.0).astype(jnp.bfloat16)
    level = sides.astype(jnp.float32).astype(jnp.bfloat16)
    side_row = jnp.where(lax.rem(sides, 2) == 0, 0.0, far_x).astype(jnp.bfloat16)
    top = jnp.where(sides < 2, 1.0, 0.0).astype(jnp.bfloat16)

    def hot(ref, line, at=0, rows=core):
        first, second = rows == row(ref, at, line), rows == row(ref, at + 1, line)
        high = jnp.where(first, row(ref, at + 2, line), jnp.where(second, row(ref, at + 4, line), zero))
        low = jnp.where(first, row(ref, at + 3, line), jnp.where(second, row(ref, at + 5, line), zero))
        return high.reshape(-1, 128), low.reshape(-1, 128)

    def across(piece, store):
        for line in range(span):
            store(piece * span + line)

    def build_ghost(line):
        high, low = hot(weigh, line, 8, banded)
        glhs[line, pl.ds(0, 2 * band)] = high
        glhs[line, pl.ds(2 * band, 2 * band)] = low

    def build_x(line):
        high, low = hot(rows_x, line)
        xrhs[line, pl.ds(0, CX)] = high
        xrhs[line, pl.ds(CX, CX)] = low
        match = side_row == row(rows_x, 1, line)
        pick = jnp.where(top > zero, row(rows_x, 4, line), row(rows_x, 5, line))
        crhs[line] = jnp.where(match, pick, zero).reshape(16, 128)

    def build_z(line):
        high, low = hot(rows_z, line)
        zrhs[line, pl.ds(0, CZ)] = high
        zrhs[line, pl.ds(CZ, CZ)] = low

    def wide(ref, start, width):
        return jnp.concatenate([ref[start + line] for line in range(width)], axis=1)

    def total(terms):
        sums = None
        for term in terms:
            sums = term if sums is None else sums + term
        return sums

    accz[...] = jnp.zeros_like(accz)
    accc[...] = jnp.zeros_like(accc)
    step = span // 2

    def prepare(piece, carry):
        across(piece, build_x)
        across(piece, build_ghost)
        across(piece, build_z)
        for side in range(2):
            start = piece * span + side * step
            accz[side] += nt_dot(wide(glhs, start, step), wide(xrhs, start, step))
        accc[...] += nt_dot(wide(glhs, piece * span, span), wide(crhs, piece * span, span))
        return carry

    lax.fori_loop(0, pieces, prepare, 0)
    fold_z[:, :CX] = gather(accz[0] + accz[1], 2 * band)
    ends = accc[pl.ds(0, 2 * band)] + accc[pl.ds(2 * band, 2 * band)]
    fold_z[:, CX:] = jnp.zeros((2 * band, CX), jnp.float32)
    fold_z[:, CX : CX + 2] = ends[:, :2] + ends[:, 2:4]
    z_copies = [
        pltpu.make_async_remote_copy(
            src_ref=fold_z.at[pl.ds(side * band, band)],
            dst_ref=zin.at[side],
            send_sem=z_send.at[side],
            recv_sem=z_recv.at[side],
            device_id={"gz": z_next[side]},
            device_id_type=MESH,
        )
        for side in range(2)
    ]
    pl.semaphore_wait(barrier, groups + 3)
    for copy in z_copies:
        copy.start()

    def paint_rows(first, second):
        for index, y in enumerate((first, second)):
            wy = jnp.where(spot[0] == y, spot[2], jnp.where(spot[1] == y, spot[3], 0.0))
            for place, value in enumerate(parts(spot[4] * wy) + parts(spot[5] * wy)):
                weigh[4 * index + place] = value

        def build(line):
            near, far = core == row(rows_x, 0, line), core == row(rows_x, 1, line)
            for index in range(2):
                for part in range(2):
                    value = jnp.where(near, row(weigh, 4 * index + part, line), jnp.where(far, row(weigh, 4 * index + 2 + part, line), zero))
                    lhs[line, pl.ds((2 * index + part) * CX, CX)] = value.reshape(CX, 128)
            pick = zero
            for index in reversed(range(4)):
                pick = jnp.where(level < jnp.bfloat16(2 * index + 2), row(weigh, 4 * (index // 2) + 2 + index % 2, line), pick)
            pick = jnp.where(edge_row == row(rows_x, 1, line), pick, zero)
            lhs[line, pl.ds(2 * BODY, 16)] = pick.reshape(16, 128)

        terms = []
        for piece in range(pieces):
            across(piece, build)
            terms.append(nt_dot(wide(lhs, piece * span, span), wide(zrhs, piece * span, span)))
        sums = total(terms)
        edges = sums[2 * BODY :, :128] + sums[2 * BODY :, 128:]
        return gather(sums[: 2 * CX], CX), gather(sums[2 * CX : 2 * BODY], CX), edges

    lane = lax.broadcasted_iota(jnp.int32, (CX, CZ), 1)
    band_row = lax.broadcasted_iota(jnp.int32, (CX, band), 1)
    edge_lane = lax.broadcasted_iota(jnp.int32, (1, CZ), 1)
    half = groups // 2
    upper = gx // half

    def pencil_of(turn):
        mine = upper * (groups - 1) + (1 - 2 * upper) * gx
        near_by = turn - (groups - half)
        near_by = near_by + jnp.where(near_by >= mine, 1, 0)
        place = jnp.where(turn < groups - half, half + turn, jnp.where(turn == groups - 1, mine, near_by))
        return upper * (groups - 1) + (1 - 2 * upper) * place

    def part_copy(target, part):
        size = CX if part is not YP else 8
        here = pl.ds(pl.multiple_of(part * CX, 8), size)
        return pltpu.make_async_remote_copy(
            src_ref=pen.at[target, here],
            dst_ref=out_ref.at[gx, here],
            send_sem=x_send.at[part, target],
            recv_sem=x_recv.at[part, gx],
            device_id={"gx": target},
            device_id_type=MESH,
        )

    y_copies = [
        pltpu.make_async_remote_copy(
            src_ref=yout.at[pl.ds(side * CX, CX)],
            dst_ref=yin.at[side],
            send_sem=y_send.at[side],
            recv_sem=y_recv.at[side],
            device_id={"gy": y_next[side]},
            device_id_type=MESH,
        )
        for side in range(2)
    ] + [
        pltpu.make_async_remote_copy(
            src_ref=yout.at[pl.ds(BODY, 8)],
            dst_ref=yin.at[2 + side, pl.ds(0, 8)],
            send_sem=y_send.at[2 + side],
            recv_sem=y_recv.at[2 + side],
            device_id={"gy": y_next[side]},
            device_id_type=MESH,
        )
        for side in range(2)
    ]
    yout[pl.ds(BODY, 8)] = jnp.zeros((8, CZ), jnp.float32)
    for target in range(groups):
        pen[target, pl.ds(BODY, 8)] = jnp.zeros((8, CZ), jnp.float32)

    def fold_into(target, rows, indices):
        edges = rows[2]
        for place, index in enumerate(indices):
            sides = [
                jnp.sum(jnp.where(band_row == index, columns[side], 0.0), axis=1, keepdims=True) for side in range(2)
            ]
            ghosts = jnp.where(lane == CZ - 1, sides[0], jnp.where(lane == 0, sides[1], 0.0))
            target[pl.ds(place * CX, CX)] = rows[place] + ghosts
            ends = [corner[side, pl.ds(index, 1)] for side in range(2)]
            for side in range(2):
                at = 4 * place + side
                value = edges[at : at + 1] + edges[at + 2 : at + 3]
                value = value + jnp.where(edge_lane == CZ - 1, ends[0][:, side : side + 1], 0.0)
                value = value + jnp.where(edge_lane == 0, ends[1][:, side : side + 1], 0.0)
                target[pl.ds(BODY + 2 * side + place, 1)] = value

    def add_first():
        pen[0, pl.ds(0, CX)] += yin[1]
        for side in range(2):
            pen[0, pl.ds(BODY + 2 * side, 1)] += yin[3, pl.ds(2 * side + 1, 1)]

    def add_last():
        pen[groups - 1, pl.ds((YP - 1) * CX, CX)] += yin[0]
        for side in range(2):
            pen[groups - 1, pl.ds(BODY + 2 * side + YP - 1, 1)] += yin[2, pl.ds(2 * side, 1)]

    late = groups - half

    def visit(turn, carry):
        ghost = turn == 1
        order = jnp.where(turn == 0, 0, turn - 1)
        target = pencil_of(order)
        first = jnp.where(ghost, 0, 1 + target * YP)
        second = jnp.where(ghost, padded_y - 1, 2 + target * YP)
        rows = paint_rows(first.astype(jnp.float32), second.astype(jnp.float32))

        @pl.when(turn == 0)
        def _():
            for copy in z_copies:
                copy.wait()
            for side in range(2):
                columns[side] = zin[side, :, pl.ds(0, CX)].T
                corner[side] = zin[side, :, pl.ds(CX, CX)]

        @pl.when(ghost)
        def _():
            fold_into(yout, rows, (first, second))
            for copy in y_copies:
                copy.start()

        @pl.when(jnp.logical_not(ghost))
        def _():
            fold_into(pen.at[target], rows, (first, second))

            @pl.when(turn > late)
            def _():
                @pl.when(turn == late + 1)
                def _():
                    for copy in y_copies:
                        copy.wait()

                @pl.when(jnp.logical_or(target == 0, jnp.logical_and(turn == late + 1, upper == 1)))
                def _():
                    add_first()

                @pl.when(jnp.logical_or(target == groups - 1, jnp.logical_and(turn == late + 1, upper == 0)))
                def _():
                    add_last()

                @pl.when(turn == late + 1)
                def _():
                    held = (1 - upper) * (groups - 1)
                    part_copy(held, (1 - upper) * (YP - 1)).start()
                    part_copy(held, YP).start()

            @pl.when(turn < groups)
            def _():
                @pl.when(turn == late)
                def _():
                    part_copy(target, upper * (YP - 1)).start()

                @pl.when(turn != late)
                def _():
                    for part in range(YP + 1):
                        part_copy(target, part).start()

        return carry

    lax.fori_loop(0, groups + 1, visit, 0)
    out_ref[gx] = pen[gx]
    for step in range(1, groups):
        source = lax.rem(gx + step, groups)
        for part in range(YP + 1):
            here = pl.ds(part * CX, CX if part < YP else 8)
            part_copy(source, part).wait_send()
            pltpu.make_async_remote_copy(
                src_ref=pen.at[source, here],
                dst_ref=out_ref.at[source, here],
                send_sem=x_send.at[part, source],
                recv_sem=x_recv.at[part, source],
                device_id={"gx": source},
                device_id_type=MESH,
            ).wait_recv()


def paint(dims, cell, offs, mass, live):
    groups = dims[0]
    lines = cell.shape[0]
    band = up(YP * groups + 2, 16)
    work = 2 * (YP * groups + 2) * 4 * CX * CZ * lines * 128
    vmem = pl.BlockSpec(memory_space=pltpu.VMEM)
    dma = pltpu.SemaphoreType.DMA
    return pl.pallas_call(
        functools.partial(paint_kernel, dims),
        out_shape=jax.ShapeDtypeStruct((groups, ROWS, CZ), jnp.float32),
        in_specs=[pl.BlockSpec(memory_space=pltpu.SMEM)] + [pl.BlockSpec(memory_space=pltpu.HBM)] * 3,
        out_specs=vmem,
        scratch_shapes=[
            pltpu.VMEM((lines, 128), jnp.int32),
            pltpu.VMEM((3, lines, 128), jnp.float32),
            pltpu.VMEM((lines, 128), jnp.float32),
            pltpu.VMEM((6, lines, 128), jnp.float32),
            pltpu.VMEM((6, lines, 128), jnp.float32),
            pltpu.VMEM((14, lines, 128), jnp.float32),
            pltpu.VMEM((6, lines, 128), jnp.float32),
            pltpu.VMEM((lines, 2 * CZ, 128), jnp.bfloat16),
            pltpu.VMEM((lines, 2 * CX, 128), jnp.bfloat16),
            pltpu.VMEM((lines, 2 * BODY + 16, 128), jnp.bfloat16),
            pltpu.VMEM((lines, 4 * band, 128), jnp.bfloat16),
            pltpu.VMEM((lines, 16, 128), jnp.bfloat16),
            pltpu.VMEM((2, 4 * band, 256), jnp.float32),
            pltpu.VMEM((4 * band, 16), jnp.float32),
            pltpu.VMEM((2, CX, band), jnp.float32),
            pltpu.VMEM((2, band, CX), jnp.float32),
            pltpu.VMEM((2 * band, 2 * CX), jnp.float32),
            pltpu.VMEM((2, band, 2 * CX), jnp.float32),
            pltpu.VMEM((ROWS, CZ), jnp.float32),
            pltpu.VMEM((4, CX, CZ), jnp.float32),
            pltpu.VMEM((groups, ROWS, CZ), jnp.float32),
            dma((3,)),
            dma((2,)),
            dma((2,)),
            dma((4,)),
            dma((4,)),
            dma((YP + 1, groups)),
            dma((YP + 1, groups)),
        ],
        cost_estimate=pl.CostEstimate(flops=work, bytes_accessed=24 * lines * 128, transcendentals=0),
        compiler_params=pltpu.CompilerParams(
            collective_id=0, has_side_effects=True, vmem_limit_bytes=32 * 1024 * 1024
        ),
    )(live, *(pltpu.with_memory_space_constraint(value, pltpu.HBM) for value in (cell, offs, mass)))


def wave_kernel(groups, in_ref, table, dens_ref, spec_ref, flat):
    length = groups * CX
    row_id = lax.broadcasted_iota(jnp.int32, (CX, CZ), 0)
    for block in range(groups):
        before, after = (block - 1) % groups, (block + 1) % groups
        for row in range(YP):
            value = in_ref[block, row * CX : (row + 1) * CX]
            upper = BODY + 2 + row
            value = value + jnp.where(row_id == 0, in_ref[before, upper : upper + 1], 0.0)
            lower = BODY + row
            value = value + jnp.where(row_id == CX - 1, in_ref[after, lower : lower + 1], 0.0)
            dens_ref[pl.ds(block * BODY + row, CX, stride=YP), :] = value
            high, low = split(value)
            flat[0, pl.ds(block * CX, CX), pl.ds(row * CZ, CZ)] = high
            flat[1, pl.ds(block * CX, CX), pl.ds(row * CZ, CZ)] = low
    tile = 256

    def transform(turn, carry):
        start = pl.multiple_of(turn * tile, tile)
        rows = pl.ds(start, tile)
        both = jnp.dot(table[0, rows, :], flat[0], preferred_element_type=jnp.float32)
        both += jnp.dot(table[1, rows, :], flat[0], preferred_element_type=jnp.float32)
        both += jnp.dot(table[0, rows, :], flat[1], preferred_element_type=jnp.float32)
        for row in range(YP):
            spec_ref[pl.ds(start * YP + row, tile, stride=YP), :] = both[:, row * CZ : (row + 1) * CZ]
        return carry

    lax.fori_loop(0, length // tile, transform, 0)


def waves(groups, pencils):
    length = groups * CX
    half = length // 2
    angle = (np.arange(half)[:, None] * np.arange(length)[None, :] % length) * (2.0 * np.pi / length)
    table = np.concatenate([np.cos(angle), -np.sin(angle)]) / np.sqrt(length)
    fhi = table.astype(jnp.bfloat16)
    flo = (table - fhi.astype(np.float64)).astype(jnp.bfloat16)
    vmem = pl.BlockSpec(memory_space=pltpu.VMEM)
    return pl.pallas_call(
        functools.partial(wave_kernel, groups),
        out_shape=[
            jax.ShapeDtypeStruct((length * YP, CZ), jnp.float32),
            jax.ShapeDtypeStruct((2 * half * YP, CZ), jnp.float32),
        ],
        in_specs=[vmem] * 2,
        out_specs=[vmem] * 2,
        scratch_shapes=[pltpu.VMEM((2, length, YP * CZ), jnp.bfloat16)],
        compiler_params=pltpu.CompilerParams(vmem_limit_bytes=24 * 1024 * 1024),
    )(pencils, jnp.asarray(np.stack([fhi, flo])))


def body(dims, cell_index, offsets, mass, counts):
    length = dims[0] * CX
    pencils = paint(
        dims, cell_index.reshape(-1, 128), offsets.reshape(3, -1, 128), mass.reshape(-1, 128), counts.reshape(1)
    )
    density, spectrum = waves(dims[0], pencils)
    return (density.reshape(length, 1, YP, CZ), spectrum.reshape(2, length // 2, 1, YP, CZ))


def solution(mesh):
    dims = tuple(mesh.shape[axis] for axis in ("gx", "gy", "gz"))
    placed = (
        P("gx", "gy", "gz", None),
        P("gx", "gy", "gz", None, None),
        P("gx", "gy", "gz", None),
        P("gx", "gy", "gz"),
    )
    return jax.shard_map(
        functools.partial(body, dims),
        mesh=mesh,
        in_specs=placed,
        out_specs=(P(None, "gx", "gy", "gz"), P(None, None, "gx", "gy", "gz")),
        check_vma=False,
    )
```

```python
import functools
import math

import jax
import jax.numpy as jnp
import numpy as np
from jax import lax
from jax.experimental import pallas as pl
from jax.experimental.pallas import tpu as pltpu
from jax.sharding import PartitionSpec as P

MESH = pl.DeviceIdType.MESH
CX = 128
YP = 2
CZ = 128


def up(n, m):
    return -(-n // m) * m


def split(value):
    high = value.astype(jnp.bfloat16)
    low = (value - high.astype(jnp.float32)).astype(jnp.bfloat16)
    return high, low


def nt_dot(lhs, rhs):
    return lax.dot_general(lhs, rhs, (((1,), (1,)), ((), ())), preferred_element_type=jnp.float32)


def gather(full, rows):
    return (full[:rows, :128] + full[rows:, :128]) + (full[:rows, 128:] + full[rows:, 128:])


BODY = YP * CX
ROWS = BODY + 8


def parts(value):
    high = value.astype(jnp.bfloat16).astype(jnp.float32)
    return high, value - high


def paint_kernel(dims, live_ref, cell_hbm, off_hbm, mass_hbm, out_ref, cell_ref, off_ref, mass_ref, rows_x, rows_z, weigh, spot, zrhs, xrhs, lhs, glhs, crhs, fold_z, zin, yout, yin, pen, load, z_send, z_recv, y_send, y_recv, x_send, x_recv):
    groups, count_y, count_z = dims
    padded_y = YP * groups + 2
    band = up(padded_y, 16)
    loads = [
        pltpu.make_async_copy(source, target, load.at[index])
        for index, (source, target) in enumerate(((cell_hbm, cell_ref), (off_hbm, off_ref), (mass_hbm, mass_ref)))
    ]
    for copy in loads:
        copy.start()
    stride_y = CZ + 2
    stride_x = padded_y * stride_y
    lines = cell_ref.shape[0]
    span = min(16, lines)
    pieces = lines // span
    gx, gy, gz = lax.axis_index("gx"), lax.axis_index("gy"), lax.axis_index("gz")
    y_next = (lax.rem(gy + count_y - 1, count_y), lax.rem(gy + 1, count_y))
    z_next = (lax.rem(gz + count_z - 1, count_z), lax.rem(gz + 1, count_z))
    barrier = pltpu.get_barrier_semaphore()
    for other in z_next:
        pl.semaphore_signal(barrier, inc=1, device_id={"gz": other}, device_id_type=MESH)
    for other in y_next:
        pl.semaphore_signal(barrier, inc=1, device_id={"gy": other}, device_id_type=MESH)
    for step in range(1, groups):
        pl.semaphore_signal(barrier, inc=1, device_id={"gx": lax.rem(gx + step, groups)}, device_id_type=MESH)

    for copy in loads:
        copy.wait()
    live = live_ref[0]
    slot = lax.broadcasted_iota(jnp.int32, (lines, 128), 0) * 128 + lax.broadcasted_iota(jnp.int32, (lines, 128), 1)
    loaded = jnp.where(slot < live, mass_ref[...], 0.0)
    cell = cell_ref[...].astype(jnp.float32)
    x0 = jnp.floor((cell + 0.5) * (1.0 / stride_x))
    rest = cell - x0 * stride_x
    y0 = jnp.floor((rest + 0.5) * (1.0 / stride_y))
    z0 = rest - y0 * stride_y
    dx, dy, dz = off_ref[0], off_ref[1], off_ref[2]
    x1 = x0 + jnp.where(dx >= 0.0, 1.0, -1.0)
    y1 = y0 + jnp.where(dy >= 0.0, 1.0, -1.0)
    z1 = z0 + jnp.where(dz >= 0.0, 1.0, -1.0)
    fx, fy, fz = jnp.abs(dx), jnp.abs(dy), jnp.abs(dz)
    ex, ey, ez = 1.0 - fx, 1.0 - fy, 1.0 - fz
    my0, my1 = ey * loaded, fy * loaded
    spot[0], spot[1], spot[2], spot[3] = y0, y1, my0, my1
    spot[4], spot[5] = ex, fx
    for index, value in enumerate((x0, x1) + parts(ex) + parts(fx)):
        rows_x[index] = value
    for index, value in enumerate((z0, z1) + parts(ez) + parts(fz)):
        rows_z[index] = value
    far_x, far_z = CX + 1.0, CZ + 1.0
    gz_y = jnp.where(z1 == 0.0, 0.0, jnp.where(z1 == far_z, float(band), -1.0 - band))
    ghost_rows = (gz_y + y0, gz_y + y1) + parts(fz * my0) + parts(fz * my1)
    for index, value in enumerate(ghost_rows):
        weigh[8 + index] = value

    def row(ref, index, line):
        value = ref[index, pl.ds(line, 1), :]
        return jnp.broadcast_to(value, (16, 128)).astype(jnp.bfloat16)[None]

    zero = jnp.zeros((1, 16, 128), jnp.bfloat16)
    count = lax.broadcasted_iota(jnp.int32, (CX // 16, 16, 128), 0) * 16 + lax.broadcasted_iota(jnp.int32, (CX // 16, 16, 128), 1)
    core = (count + 1).astype(jnp.float32).astype(jnp.bfloat16)
    banded = count.astype(jnp.float32).astype(jnp.bfloat16)[: 2 * band // 16]
    sides = lax.broadcasted_iota(jnp.int32, (1, 16, 128), 1)
    edge_row = jnp.where(sides < 4 * YP, jnp.where(lax.rem(sides, 2) == 0, 0.0, far_x), -9.0).astype(jnp.bfloat16)
    level = sides.astype(jnp.float32).astype(jnp.bfloat16)
    side_row = jnp.where(lax.rem(sides, 2) == 0, 0.0, far_x).astype(jnp.bfloat16)
    top = jnp.where(sides < 2, 1.0, 0.0).astype(jnp.bfloat16)

    def hot(ref, line, at=0, rows=core):
        first, second = rows == row(ref, at, line), rows == row(ref, at + 1, line)
        high = jnp.where(first, row(ref, at + 2, line), jnp.where(second, row(ref, at + 4, line), zero))
        low = jnp.where(first, row(ref, at + 3, line), jnp.where(second, row(ref, at + 5, line), zero))
        return high.reshape(-1, 128), low.reshape(-1, 128)

    def across(piece, store):
        for line in range(span):
            store(piece * span + line)

    def build_ghost(line):
        high, low = hot(weigh, line, 8, banded)
        glhs[line, pl.ds(0, 2 * band)] = high
        glhs[line, pl.ds(2 * band, 2 * band)] = low

    def build_x(line):
        high, low = hot(rows_x, line)
        xrhs[line, pl.ds(0, CX)] = high
        xrhs[line, pl.ds(CX, CX)] = low
        match = side_row == row(rows_x, 1, line)
        pick = jnp.where(top > zero, row(rows_x, 4, line), row(rows_x, 5, line))
        crhs[line] = jnp.where(match, pick, zero).reshape(16, 128)

    def build_z(line):
        high, low = hot(rows_z, line)
        zrhs[line, pl.ds(0, CZ)] = high
        zrhs[line, pl.ds(CZ, CZ)] = low

    def wide(ref, start, width):
        return jnp.concatenate([ref[start + line] for line in range(width)], axis=1)

    def total(terms):
        sums = None
        for term in terms:
            sums = term if sums is None else sums + term
        return sums

    def paint_rows(first, second):
        for index, y in enumerate((first, second)):
            wy = jnp.where(spot[0] == y, spot[2], jnp.where(spot[1] == y, spot[3], 0.0))
            for place, value in enumerate(parts(spot[4] * wy) + parts(spot[5] * wy)):
                weigh[4 * index + place] = value

        def build(line):
            near, far = core == row(rows_x, 0, line), core == row(rows_x, 1, line)
            for index in range(2):
                for part in range(2):
                    value = jnp.where(near, row(weigh, 4 * index + part, line), jnp.where(far, row(weigh, 4 * index + 2 + part, line), zero))
                    lhs[line, pl.ds((2 * index + part) * CX, CX)] = value.reshape(CX, 128)
            pick = zero
            for index in reversed(range(4)):
                pick = jnp.where(level < jnp.bfloat16(2 * index + 2), row(weigh, 4 * (index // 2) + 2 + index % 2, line), pick)
            pick = jnp.where(edge_row == row(rows_x, 1, line), pick, zero)
            lhs[line, pl.ds(2 * BODY, 16)] = pick.reshape(16, 128)

        terms = []
        for piece in range(pieces):
            across(piece, build)
            terms.append(nt_dot(wide(lhs, piece * span, span), wide(zrhs, piece * span, span)))
        sums = total(terms)
        edges = sums[2 * BODY :, :128] + sums[2 * BODY :, 128:]
        return gather(sums[: 2 * CX], CX), gather(sums[2 * CX : 2 * BODY], CX), edges

    edge_lane = lax.broadcasted_iota(jnp.int32, (1, CZ), 1)
    half = groups // 2
    upper = gx // half

    def pencil_of(turn):
        mine = upper * (groups - 1) + (1 - 2 * upper) * gx
        near_by = turn - (groups - half)
        near_by = near_by + jnp.where(near_by >= mine, 1, 0)
        place = jnp.where(turn < groups - half, half + turn, jnp.where(turn == groups - 1, mine, near_by))
        return upper * (groups - 1) + (1 - 2 * upper) * place

    def part_copy(target, part):
        size = CX if part is not YP else 8
        here = pl.ds(pl.multiple_of(part * CX, 8), size)
        return pltpu.make_async_remote_copy(
            src_ref=pen.at[target, here],
            dst_ref=out_ref.at[gx, here],
            send_sem=x_send.at[part, target],
            recv_sem=x_recv.at[part, gx],
            device_id={"gx": target},
            device_id_type=MESH,
        )

    y_copies = [
        pltpu.make_async_remote_copy(
            src_ref=yout.at[pl.ds(side * CX, CX)],
            dst_ref=yin.at[side],
            send_sem=y_send.at[side],
            recv_sem=y_recv.at[side],
            device_id={"gy": y_next[side]},
            device_id_type=MESH,
        )
        for side in range(2)
    ] + [
        pltpu.make_async_remote_copy(
            src_ref=yout.at[pl.ds(BODY, 8)],
            dst_ref=yin.at[2 + side, pl.ds(0, 8)],
            send_sem=y_send.at[2 + side],
            recv_sem=y_recv.at[2 + side],
            device_id={"gy": y_next[side]},
            device_id_type=MESH,
        )
        for side in range(2)
    ]
    def put(target, place, rows, at):
        edges = rows[YP]
        target[pl.ds(pl.multiple_of(place * CX, 8), CX)] = rows[at]
        for side in range(2):
            low = 4 * at + side
            target[pl.ds(BODY + 2 * side + place, 1)] = edges[low : low + 1] + edges[low + 2 : low + 3]

    def finish(target, place, index):
        ends = [zin[side, 1, pl.ds(index, 1)] for side in range(2)]
        for side in range(2):
            extra = jnp.where(edge_lane == CZ - 1, ends[0][:, side : side + 1], 0.0)
            extra = extra + jnp.where(edge_lane == 0, ends[1][:, side : side + 1], 0.0)
            target[pl.ds(BODY + 2 * side + place, 1)] += extra
            target[pl.ds(BODY + 4 + 2 * side + place, 1)] = zin[side, 0, pl.ds(index, 1)]

    def add_first():
        pen[0, pl.ds(0, CX)] += yin[1]
        for kind in range(4):
            pen[0, pl.ds(BODY + 2 * kind, 1)] += yin[3, pl.ds(2 * kind + 1, 1)]

    def add_last():
        pen[groups - 1, pl.ds((YP - 1) * CX, CX)] += yin[0]
        for kind in range(4):
            pen[groups - 1, pl.ds(BODY + 2 * kind + YP - 1, 1)] += yin[2, pl.ds(2 * kind, 1)]

    late = groups - half

    def line_of(target, place):
        return 1 + target * YP + place

    def as_float(indices):
        return [index.astype(jnp.float32) for index in indices]

    def build_all(piece, carry):
        across(piece, build_z)
        return carry

    lax.fori_loop(0, pieces, build_all, 0)
    leader = pencil_of(jnp.int32(0))
    rows = paint_rows(*as_float([line_of(leader, place) for place in range(YP)]))
    for place in range(YP):
        put(pen.at[leader], place, rows, place)
    pl.semaphore_wait(barrier, groups + 3)
    for part in range(YP):
        part_copy(leader, part).start()

    z_copies = [
        pltpu.make_async_remote_copy(
            src_ref=fold_z.at[side],
            dst_ref=zin.at[side],
            send_sem=z_send.at[side],
            recv_sem=z_recv.at[side],
            device_id={"gz": z_next[side]},
            device_id_type=MESH,
        )
        for side in range(2)
    ]
    def send_ghosts():
        step = pieces // 2
        sums = []
        for piece in range(pieces):
            across(piece, build_x)
            across(piece, build_ghost)
        for side in range(2):
            starts = [piece * span for piece in range(side * step, step if side == 0 else pieces)]
            sums.append(total(nt_dot(wide(glhs, start, span), wide(xrhs, start, span)) for start in starts))
        ends = total(nt_dot(wide(glhs, piece * span, span), wide(crhs, piece * span, span)) for piece in range(pieces))
        sums = gather(sums[0] + sums[1], 2 * band)
        ends = ends[: 2 * band] + ends[2 * band :]
        ends = ends[:, :2] + ends[:, 2:4]
        for side in range(2):
            here = slice(side * band, side * band + band)
            fold_z[side, 0] = sums[here]
            fold_z[side, 1] = jnp.zeros((band, CX), jnp.float32)
            fold_z[side, 1, :, pl.ds(0, 2)] = ends[here]
        for copy in z_copies:
            copy.start()

    pl.when(gx >= 0)(send_ghosts)
    held, close = pencil_of(jnp.int32(late - 1)), pencil_of(jnp.int32(late))

    def visit(turn, carry):
        ghost = turn == 1
        whole = pencil_of(turn - 1)
        early, second = turn == late, turn == late + 1
        split_turn = jnp.logical_or(early, second)
        targets = (jnp.where(split_turn, held, whole), jnp.where(split_turn, close, whole))
        places = (
            jnp.where(early, upper, jnp.where(second, 1 - upper, 0)),
            jnp.where(early, 1 - upper, jnp.where(second, upper, 1)),
        )
        lines = [line_of(target, place) for target, place in zip(targets, places)]
        lines = (jnp.where(ghost, 0, lines[0]), jnp.where(ghost, padded_y - 1, lines[1]))
        rows = paint_rows(*as_float(lines))

        @pl.when(ghost)
        def _():
            for place in range(YP):
                put(yout, place, rows, place)
            for copy in z_copies:
                copy.wait()
            for place, line in enumerate(lines):
                finish(yout, place, line)
            for copy in y_copies:
                copy.start()
            for place in range(YP):
                finish(pen.at[leader], place, line_of(leader, place))
            part_copy(leader, YP).start()

        @pl.when(jnp.logical_not(ghost))
        def _():
            for at, (target, place) in enumerate(zip(targets, places)):
                put(pen.at[target], place, rows, at)

            @pl.when(early)
            def _():
                for target, place in zip(targets, places):
                    part_copy(target, place).start()

            for target, place, line in zip(targets, places, lines):
                finish(pen.at[target], place, line)

            @pl.when(second)
            def _():
                for copy in y_copies:
                    copy.wait()

            @pl.when(jnp.logical_or(jnp.logical_and(second, gx != 0), jnp.logical_and(turn == groups, gx == 0)))
            def _():
                add_first()

            @pl.when(
                jnp.logical_or(
                    jnp.logical_and(second, gx != groups - 1), jnp.logical_and(turn == groups, gx == groups - 1)
                )
            )
            def _():
                add_last()

            @pl.when(jnp.logical_and(turn < groups, jnp.logical_not(early)))
            def _():
                for target, place in zip(targets, places):
                    part_copy(target, place).start()
                part_copy(targets[0], YP).start()

            @pl.when(second)
            def _():
                part_copy(close, YP).start()

        return carry

    lax.fori_loop(1, groups + 1, visit, 0)
    out_ref[gx] = pen[gx]
    for step in range(1, groups):
        source = lax.rem(gx + step, groups)
        for part in range(YP + 1):
            here = pl.ds(part * CX, CX if part < YP else 8)
            part_copy(source, part).wait_send()
            pltpu.make_async_remote_copy(
                src_ref=pen.at[source, here],
                dst_ref=out_ref.at[source, here],
                send_sem=x_send.at[part, source],
                recv_sem=x_recv.at[part, source],
                device_id={"gx": source},
                device_id_type=MESH,
            ).wait_recv()


def paint(dims, cell, offs, mass, live):
    groups = dims[0]
    lines = cell.shape[0]
    band = up(YP * groups + 2, 16)
    work = 2 * (YP * groups + 2) * 4 * CX * CZ * lines * 128
    vmem = pl.BlockSpec(memory_space=pltpu.VMEM)
    dma = pltpu.SemaphoreType.DMA
    return pl.pallas_call(
        functools.partial(paint_kernel, dims),
        out_shape=jax.ShapeDtypeStruct((groups, ROWS, CZ), jnp.float32),
        in_specs=[pl.BlockSpec(memory_space=pltpu.SMEM)] + [pl.BlockSpec(memory_space=pltpu.HBM)] * 3,
        out_specs=vmem,
        scratch_shapes=[
            pltpu.VMEM((lines, 128), jnp.int32),
            pltpu.VMEM((3, lines, 128), jnp.float32),
            pltpu.VMEM((lines, 128), jnp.float32),
            pltpu.VMEM((6, lines, 128), jnp.float32),
            pltpu.VMEM((6, lines, 128), jnp.float32),
            pltpu.VMEM((14, lines, 128), jnp.float32),
            pltpu.VMEM((6, lines, 128), jnp.float32),
            pltpu.VMEM((lines, 2 * CZ, 128), jnp.bfloat16),
            pltpu.VMEM((lines, 2 * CX, 128), jnp.bfloat16),
            pltpu.VMEM((lines, 2 * BODY + 16, 128), jnp.bfloat16),
            pltpu.VMEM((lines, 4 * band, 128), jnp.bfloat16),
            pltpu.VMEM((lines, 16, 128), jnp.bfloat16),
            pltpu.VMEM((2, 2, band, CX), jnp.float32),
            pltpu.VMEM((2, 2, band, CX), jnp.float32),
            pltpu.VMEM((ROWS, CZ), jnp.float32),
            pltpu.VMEM((4, CX, CZ), jnp.float32),
            pltpu.VMEM((groups, ROWS, CZ), jnp.float32),
            dma((3,)),
            dma((2,)),
            dma((2,)),
            dma((4,)),
            dma((4,)),
            dma((YP + 1, groups)),
            dma((YP + 1, groups)),
        ],
        cost_estimate=pl.CostEstimate(flops=work, bytes_accessed=24 * lines * 128, transcendentals=0),
        compiler_params=pltpu.CompilerParams(
            collective_id=0, has_side_effects=True, vmem_limit_bytes=32 * 1024 * 1024
        ),
    )(live, *(pltpu.with_memory_space_constraint(value, pltpu.HBM) for value in (cell, offs, mass)))


def wave_kernel(groups, in_ref, table, dens_ref, spec_ref, flat):
    length = groups * CX
    row_id = lax.broadcasted_iota(jnp.int32, (CX, CZ), 0)
    lane = lax.broadcasted_iota(jnp.int32, (CX, CZ), 1)
    columns = jnp.concatenate([in_ref[block, BODY:ROWS] for block in range(groups)], axis=0).T
    for block in range(groups):
        before, after = (block - 1) % groups, (block + 1) % groups
        for row in range(YP):
            value = in_ref[block, row * CX : (row + 1) * CX]
            upper = BODY + 2 + row
            value = value + jnp.where(row_id == 0, in_ref[before, upper : upper + 1], 0.0)
            lower = BODY + row
            value = value + jnp.where(row_id == CX - 1, in_ref[after, lower : lower + 1], 0.0)
            ends = [columns[:, 8 * block + 4 + 2 * side + row :][:, :1] for side in range(2)]
            value = value + jnp.where(lane == CZ - 1, ends[0], jnp.where(lane == 0, ends[1], 0.0))
            dens_ref[pl.ds(block * BODY + row, CX, stride=YP), :] = value
            high, low = split(value)
            flat[0, pl.ds(block * CX, CX), pl.ds(row * CZ, CZ)] = high
            flat[1, pl.ds(block * CX, CX), pl.ds(row * CZ, CZ)] = low
    tile = 256

    def transform(turn, carry):
        start = pl.multiple_of(turn * tile, tile)
        rows = pl.ds(start, tile)
        both = jnp.dot(table[0, rows, :], flat[0], preferred_element_type=jnp.float32)
        both += jnp.dot(table[1, rows, :], flat[0], preferred_element_type=jnp.float32)
        both += jnp.dot(table[0, rows, :], flat[1], preferred_element_type=jnp.float32)
        for row in range(YP):
            spec_ref[pl.ds(start * YP + row, tile, stride=YP), :] = both[:, row * CZ : (row + 1) * CZ]
        return carry

    lax.fori_loop(0, length // tile, transform, 0)


def waves(groups, pencils):
    length = groups * CX
    half = length // 2
    angle = (np.arange(half)[:, None] * np.arange(length)[None, :] % length) * (2.0 * np.pi / length)
    table = np.concatenate([np.cos(angle), -np.sin(angle)]) / np.sqrt(length)
    fhi = table.astype(jnp.bfloat16)
    flo = (table - fhi.astype(np.float64)).astype(jnp.bfloat16)
    vmem = pl.BlockSpec(memory_space=pltpu.VMEM)
    return pl.pallas_call(
        functools.partial(wave_kernel, groups),
        out_shape=[
            jax.ShapeDtypeStruct((length * YP, CZ), jnp.float32),
            jax.ShapeDtypeStruct((2 * half * YP, CZ), jnp.float32),
        ],
        in_specs=[vmem] * 2,
        out_specs=[vmem] * 2,
        scratch_shapes=[pltpu.VMEM((2, length, YP * CZ), jnp.bfloat16)],
        compiler_params=pltpu.CompilerParams(vmem_limit_bytes=24 * 1024 * 1024),
    )(pencils, jnp.asarray(np.stack([fhi, flo])))


def body(dims, cell_index, offsets, mass, counts):
    length = dims[0] * CX
    pencils = paint(
        dims, cell_index.reshape(-1, 128), offsets.reshape(3, -1, 128), mass.reshape(-1, 128), counts.reshape(1)
    )
    density, spectrum = waves(dims[0], pencils)
    return (density.reshape(length, 1, YP, CZ), spectrum.reshape(2, length // 2, 1, YP, CZ))


def solution(mesh):
    dims = tuple(mesh.shape[axis] for axis in ("gx", "gy", "gz"))
    placed = (
        P("gx", "gy", "gz", None),
        P("gx", "gy", "gz", None, None),
        P("gx", "gy", "gz", None),
        P("gx", "gy", "gz"),
    )
    return jax.shard_map(
        functools.partial(body, dims),
        mesh=mesh,
        in_specs=placed,
        out_specs=(P(None, "gx", "gy", "gz"), P(None, None, "gx", "gy", "gz")),
        check_vma=False,
    )
```

```python
import functools
import math

import jax
import jax.numpy as jnp
import numpy as np
from jax import lax
from jax.experimental import pallas as pl
from jax.experimental.pallas import tpu as pltpu
from jax.sharding import PartitionSpec as P

MESH = pl.DeviceIdType.MESH
CX = 128
YP = 2
CZ = 128


def up(n, m):
    return -(-n // m) * m


def split(value):
    high = value.astype(jnp.bfloat16)
    low = (value - high.astype(jnp.float32)).astype(jnp.bfloat16)
    return high, low


def nt_dot(lhs, rhs):
    return lax.dot_general(lhs, rhs, (((1,), (1,)), ((), ())), preferred_element_type=jnp.float32)


def gather(full, rows):
    return (full[:rows, :128] + full[rows:, :128]) + (full[:rows, 128:] + full[rows:, 128:])


BODY = YP * CX
ROWS = BODY + 8


def parts(value):
    high = value.astype(jnp.bfloat16).astype(jnp.float32)
    return high, value - high


def paint_kernel(dims, live_ref, cell_hbm, off_hbm, mass_hbm, out_ref, cell_ref, off_ref, mass_ref, rows_x, rows_z, weigh, spot, zrhs, xrhs, lhs, glhs, crhs, fold_z, zin, yout, yin, fout, fin, pen, load, z_send, z_recv, y_send, y_recv, f_send, f_recv, x_send, x_recv, opened):
    groups, count_y, count_z = dims
    padded_y = YP * groups + 2
    band = up(padded_y, 16)
    loads = [
        pltpu.make_async_copy(source, target, load.at[index])
        for index, (source, target) in enumerate(((cell_hbm, cell_ref), (off_hbm, off_ref), (mass_hbm, mass_ref)))
    ]
    for copy in loads:
        copy.start()
    stride_y = CZ + 2
    stride_x = padded_y * stride_y
    lines = cell_ref.shape[0]
    span = min(16, lines)
    pieces = lines // span
    gx, gy, gz = lax.axis_index("gx"), lax.axis_index("gy"), lax.axis_index("gz")
    y_next = (lax.rem(gy + count_y - 1, count_y), lax.rem(gy + 1, count_y))
    z_next = (lax.rem(gz + count_z - 1, count_z), lax.rem(gz + 1, count_z))
    barrier = pltpu.get_barrier_semaphore()
    for other in z_next:
        pl.semaphore_signal(barrier, inc=1, device_id={"gz": other}, device_id_type=MESH)
    for other in y_next:
        pl.semaphore_signal(barrier, inc=1, device_id={"gy": other}, device_id_type=MESH)
    for step in range(1, groups):
        pl.semaphore_signal(barrier, inc=1, device_id={"gx": lax.rem(gx + step, groups)}, device_id_type=MESH)
    for copy in loads:
        copy.wait()
    live = live_ref[0]
    slot = lax.broadcasted_iota(jnp.int32, (lines, 128), 0) * 128 + lax.broadcasted_iota(jnp.int32, (lines, 128), 1)
    loaded = jnp.where(slot < live, mass_ref[...], 0.0)
    cell = cell_ref[...].astype(jnp.float32)
    x0 = jnp.floor((cell + 0.5) * (1.0 / stride_x))
    rest = cell - x0 * stride_x
    y0 = jnp.floor((rest + 0.5) * (1.0 / stride_y))
    z0 = rest - y0 * stride_y
    dx, dy, dz = off_ref[0], off_ref[1], off_ref[2]
    x1 = x0 + jnp.where(dx >= 0.0, 1.0, -1.0)
    y1 = y0 + jnp.where(dy >= 0.0, 1.0, -1.0)
    z1 = z0 + jnp.where(dz >= 0.0, 1.0, -1.0)
    fx, fy, fz = jnp.abs(dx), jnp.abs(dy), jnp.abs(dz)
    ex, ey, ez = 1.0 - fx, 1.0 - fy, 1.0 - fz
    my0, my1 = ey * loaded, fy * loaded
    spot[0], spot[1], spot[2], spot[3] = y0, y1, my0, my1
    spot[4], spot[5] = ex, fx
    for index, value in enumerate((x0, x1) + parts(ex) + parts(fx)):
        rows_x[index] = value
    for index, value in enumerate((z0, z1) + parts(ez) + parts(fz)):
        rows_z[index] = value
    far_x, far_z = CX + 1.0, CZ + 1.0
    gz_y = jnp.where(z1 == 0.0, 0.0, jnp.where(z1 == far_z, float(band), -1.0 - band))
    ghost_rows = (gz_y + y0, gz_y + y1) + parts(fz * my0) + parts(fz * my1)
    for index, value in enumerate(ghost_rows):
        weigh[8 + index] = value

    def row(ref, index, line):
        value = ref[index, pl.ds(line, 1), :]
        return jnp.broadcast_to(value, (16, 128)).astype(jnp.bfloat16)[None]

    zero = jnp.zeros((1, 16, 128), jnp.bfloat16)
    count = lax.broadcasted_iota(jnp.int32, (CX // 16, 16, 128), 0) * 16 + lax.broadcasted_iota(jnp.int32, (CX // 16, 16, 128), 1)
    core = (count + 1).astype(jnp.float32).astype(jnp.bfloat16)
    banded = count.astype(jnp.float32).astype(jnp.bfloat16)[: 2 * band // 16]
    sides = lax.broadcasted_iota(jnp.int32, (1, 16, 128), 1)
    edge_row = jnp.where(sides < 4 * YP, jnp.where(lax.rem(sides, 2) == 0, 0.0, far_x), -9.0).astype(jnp.bfloat16)
    level = sides.astype(jnp.float32).astype(jnp.bfloat16)
    side_row = jnp.where(lax.rem(sides, 2) == 0, 0.0, far_x).astype(jnp.bfloat16)
    top = jnp.where(sides < 2, 1.0, 0.0).astype(jnp.bfloat16)

    def hot(ref, line, at=0, rows=core):
        first, second = rows == row(ref, at, line), rows == row(ref, at + 1, line)
        high = jnp.where(first, row(ref, at + 2, line), jnp.where(second, row(ref, at + 4, line), zero))
        low = jnp.where(first, row(ref, at + 3, line), jnp.where(second, row(ref, at + 5, line), zero))
        return high.reshape(-1, 128), low.reshape(-1, 128)

    def across(piece, store):
        for line in range(span):
            store(piece * span + line)

    def build_ghost(line):
        high, low = hot(weigh, line, 8, banded)
        glhs[line, pl.ds(0, 2 * band)] = high
        glhs[line, pl.ds(2 * band, 2 * band)] = low

    def build_x(line):
        high, low = hot(rows_x, line)
        xrhs[line, pl.ds(0, CX)] = high
        xrhs[line, pl.ds(CX, CX)] = low
        match = side_row == row(rows_x, 1, line)
        pick = jnp.where(top > zero, row(rows_x, 4, line), row(rows_x, 5, line))
        crhs[line] = jnp.where(match, pick, zero).reshape(16, 128)

    def build_z(line):
        high, low = hot(rows_z, line)
        zrhs[line, pl.ds(0, CZ)] = high
        zrhs[line, pl.ds(CZ, CZ)] = low

    def wide(ref, start, width):
        return jnp.concatenate([ref[start + line] for line in range(width)], axis=1)

    def total(terms):
        sums = None
        for term in terms:
            sums = term if sums is None else sums + term
        return sums

    def paint_rows(first, second):
        for index, y in enumerate((first, second)):
            wy = jnp.where(spot[0] == y, spot[2], jnp.where(spot[1] == y, spot[3], 0.0))
            for place, value in enumerate(parts(spot[4] * wy) + parts(spot[5] * wy)):
                weigh[4 * index + place] = value

        def build(line):
            near, far = core == row(rows_x, 0, line), core == row(rows_x, 1, line)
            for index in range(2):
                for part in range(2):
                    value = jnp.where(near, row(weigh, 4 * index + part, line), jnp.where(far, row(weigh, 4 * index + 2 + part, line), zero))
                    lhs[line, pl.ds((2 * index + part) * CX, CX)] = value.reshape(CX, 128)
            pick = zero
            for index in reversed(range(4)):
                pick = jnp.where(level < jnp.bfloat16(2 * index + 2), row(weigh, 4 * (index // 2) + 2 + index % 2, line), pick)
            pick = jnp.where(edge_row == row(rows_x, 1, line), pick, zero)
            lhs[line, pl.ds(2 * BODY, 16)] = pick.reshape(16, 128)

        terms = []
        for piece in range(pieces):
            across(piece, build)
            terms.append(nt_dot(wide(lhs, piece * span, span), wide(zrhs, piece * span, span)))
        sums = total(terms)
        edges = sums[2 * BODY :, :128] + sums[2 * BODY :, 128:]
        return gather(sums[: 2 * CX], CX), gather(sums[2 * CX : 2 * BODY], CX), edges

    edge_lane = lax.broadcasted_iota(jnp.int32, (1, CZ), 1)
    half = groups // 2
    upper = gx // half

    def pencil_of(turn):
        mine = upper * (groups - 1) + (1 - 2 * upper) * gx
        near_by = turn - (groups - half)
        near_by = near_by + jnp.where(near_by >= mine, 1, 0)
        place = jnp.where(turn < groups - half, half + turn, jnp.where(turn == groups - 1, mine, near_by))
        return upper * (groups - 1) + (1 - 2 * upper) * place

    def part_copy(target, part):
        size = CX if part is not YP else 8
        here = pl.ds(pl.multiple_of(part * CX, 8), size)
        return pltpu.make_async_remote_copy(
            src_ref=pen.at[target, here],
            dst_ref=out_ref.at[gx, here],
            send_sem=x_send.at[part, target],
            recv_sem=x_recv.at[part, gx],
            device_id={"gx": target},
            device_id_type=MESH,
        )

    y_copies = [
        pltpu.make_async_remote_copy(
            src_ref=yout.at[side],
            dst_ref=yin.at[side],
            send_sem=y_send.at[side],
            recv_sem=y_recv.at[side],
            device_id={"gy": y_next[side]},
            device_id_type=MESH,
        )
        for side in range(2)
    ]
    far_copies = [
        pltpu.make_async_remote_copy(
            src_ref=fout.at[side],
            dst_ref=fin.at[gx],
            send_sem=f_send.at[side],
            recv_sem=f_recv.at[gx],
            device_id={"gx": jnp.int32((groups - 1) * (1 - side)), "gy": y_next[side]},
            device_id_type=MESH,
        )
        for side in range(2)
    ]

    def put(target, main, edge, pitch, rows, at):
        edges = rows[YP]
        target[pl.ds(main, CX)] = rows[at]
        for side in range(2):
            low = 4 * at + side
            target[pl.ds(edge + pitch * side, 1)] = edges[low : low + 1] + edges[low + 2 : low + 3]

    def put_pen(target, place, rows, at):
        put(pen.at[target], pl.multiple_of(place * CX, 8), BODY + place, 2, rows, at)

    def corners(index):
        ends = [zin[side, 1, pl.ds(index, 1)] for side in range(2)]
        for side in range(2):
            extra = jnp.where(edge_lane == CZ - 1, ends[0][:, side : side + 1], 0.0)
            yield extra + jnp.where(edge_lane == 0, ends[1][:, side : side + 1], 0.0)

    def finish(target, place):
        index = 1 + target * YP + place
        for side, extra in enumerate(corners(index)):
            pen[target, pl.ds(BODY + 2 * side + place, 1)] += extra
            pen[target, pl.ds(BODY + 4 + 2 * side + place, 1)] = zin[side, 0, pl.ds(index, 1)]

    def send_corners():
        for side, index in enumerate((0, padded_y - 1)):
            for kind, extra in enumerate(corners(index)):
                fout[side, pl.ds(kind, 1)] = extra
                fout[side, pl.ds(2 + kind, 1)] = zin[kind, 0, pl.ds(index, 1)]
            far_copies[side].start()

    def add_first():
        pen[0, pl.ds(0, CX)] += yin[1, pl.ds(0, CX)]
        for side in range(2):
            pen[0, pl.ds(BODY + 2 * side, 1)] += yin[1, pl.ds(CX + side, 1)]

    def add_last():
        pen[groups - 1, pl.ds((YP - 1) * CX, CX)] += yin[0, pl.ds(0, CX)]
        for side in range(2):
            pen[groups - 1, pl.ds(BODY + 2 * side + YP - 1, 1)] += yin[0, pl.ds(CX + side, 1)]

    late = groups - half

    def line_of(target, place):
        return 1 + target * YP + place

    def as_float(indices):
        return [index.astype(jnp.float32) for index in indices]

    def build_all(piece, carry):
        across(piece, build_z)
        return carry

    lax.fori_loop(0, pieces, build_all, 0)
    leader = pencil_of(jnp.int32(0))
    rows = paint_rows(*as_float([line_of(leader, place) for place in range(YP)]))
    for place in range(YP):
        put_pen(leader, place, rows, place)
    pl.semaphore_wait(barrier, groups + 3)

    @pl.when(jnp.logical_or(gx == 0, gx == groups - 1))
    def _():
        for step in range(1, groups):
            pl.semaphore_signal(
                opened, inc=1, device_id={"gx": lax.rem(gx + step, groups)}, device_id_type=MESH
            )

    for part in range(YP):
        part_copy(leader, part).start()

    z_copies = [
        pltpu.make_async_remote_copy(
            src_ref=fold_z.at[side],
            dst_ref=zin.at[side],
            send_sem=z_send.at[side],
            recv_sem=z_recv.at[side],
            device_id={"gz": z_next[side]},
            device_id_type=MESH,
        )
        for side in range(2)
    ]
    def send_ghosts():
        step = span // 2
        terms = ([], [])
        for piece in range(pieces):
            across(piece, build_x)
            across(piece, build_ghost)
            for side in range(2):
                start = piece * span + side * step
                terms[side].append(nt_dot(wide(glhs, start, step), wide(xrhs, start, step)))
        sums = [total(terms[side]) for side in range(2)]
        ends = total(nt_dot(wide(glhs, piece * span, span), wide(crhs, piece * span, span)) for piece in range(pieces))
        sums = gather(sums[0] + sums[1], 2 * band)
        ends = ends[: 2 * band] + ends[2 * band :]
        ends = ends[:, :2] + ends[:, 2:4]
        for side in range(2):
            here = slice(side * band, side * band + band)
            fold_z[side, 0] = sums[here]
            fold_z[side, 1] = jnp.zeros((band, CX), jnp.float32)
            fold_z[side, 1, :, pl.ds(0, 2)] = ends[here]
        for copy in z_copies:
            copy.start()

    yout[:, pl.ds(CX, 8)] = jnp.zeros((2, 8, CZ), jnp.float32)
    fout[...] = jnp.zeros_like(fout)
    held, close = pencil_of(jnp.int32(late - 1)), pencil_of(jnp.int32(late))

    def visit(turn, carry):
        whole = pencil_of(turn - 1)
        opening, closing, joining = turn == 1, turn == late, turn == late + 1
        first = jnp.where(joining, line_of(held, 1 - upper), line_of(whole, 0))
        second = jnp.where(joining, line_of(close, upper), line_of(whole, 1))
        first = jnp.where(opening, upper * (padded_y - 1), jnp.where(closing, line_of(close, 1 - upper), first))
        second = jnp.where(opening, line_of(held, upper), jnp.where(closing, (1 - upper) * (padded_y - 1), second))
        rows = paint_rows(*as_float((first, second)))

        @pl.when(opening)
        def _():
            put_pen(held, upper, rows, 1)
            part_copy(held, upper).start()
            put(yout.at[upper], 0, CX, 1, rows, 0)
            for side in range(2):
                pl.when(upper == side)(y_copies[side].start)

        @pl.when(closing)
        def _():
            put_pen(close, 1 - upper, rows, 0)
            part_copy(close, 1 - upper).start()
            put(yout.at[1 - upper], 0, CX, 1, rows, 1)
            for side in range(2):
                pl.when(upper == 1 - side)(y_copies[side].start)
            send_ghosts()

        @pl.when(joining)
        def _():
            put_pen(held, 1 - upper, rows, 0)
            put_pen(close, upper, rows, 1)
            for side in range(2):

                @pl.when(upper == side)
                def _():
                    y_copies[side].wait()
                    (add_first if side else add_last)()

            part_copy(held, 1 - upper).start()
            for copy in z_copies:
                copy.wait()
            pl.semaphore_wait(opened, jnp.where(jnp.logical_or(gx == 0, gx == groups - 1), 1, 2))
            send_corners()
            for order in range(late):
                target = pencil_of(jnp.int32(order))
                for place in range(YP):
                    finish(target, place)
                part_copy(target, YP).start()
            for place in range(YP):
                finish(close, place)
            for side in range(2):

                @pl.when(upper == 1 - side)
                def _():
                    y_copies[side].wait()
                    pl.when(gx != (groups - 1) * (1 - side))(add_first if side else add_last)

            part_copy(close, upper).start()
            part_copy(close, YP).start()

        @pl.when(jnp.logical_not(jnp.logical_or(opening, jnp.logical_or(closing, joining))))
        def _():
            for place in range(YP):
                put_pen(whole, place, rows, place)

            @pl.when(turn < late)
            def _():
                for place in range(YP):
                    part_copy(whole, place).start()

            @pl.when(turn > late + 1)
            def _():
                for place in range(YP):
                    finish(whole, place)

                @pl.when(turn < groups)
                def _():
                    for part in range(YP + 1):
                        part_copy(whole, part).start()

        return carry

    lax.fori_loop(1, groups + 1, visit, 0)
    pl.when(gx == 0)(add_first)
    pl.when(gx == groups - 1)(add_last)
    out_ref[gx] = pen[gx]
    for step in range(1, groups):
        source = lax.rem(gx + step, groups)
        for part in range(YP + 1):
            here = pl.ds(part * CX, CX if part < YP else 8)
            part_copy(source, part).wait_send()
            pltpu.make_async_remote_copy(
                src_ref=pen.at[source, here],
                dst_ref=out_ref.at[source, here],
                send_sem=x_send.at[part, source],
                recv_sem=x_recv.at[part, source],
                device_id={"gx": source},
                device_id_type=MESH,
            ).wait_recv()
    for side in range(2):
        far_copies[side].wait_send()
    for side, owner in enumerate((groups - 1, 0)):

        @pl.when(gx == owner)
        def _():
            for source in range(groups):
                pltpu.make_async_remote_copy(
                    src_ref=fout.at[side],
                    dst_ref=fin.at[source],
                    send_sem=f_send.at[side],
                    recv_sem=f_recv.at[source],
                    device_id={"gx": jnp.int32(source), "gy": y_next[side]},
                    device_id_type=MESH,
                ).wait_recv()
                for kind in range(4):
                    at = pl.ds(BODY + 2 * kind + (YP - 1) * (1 - side), 1)
                    out_ref[source, at] += fin[source, pl.ds(kind, 1)]


def paint(dims, cell, offs, mass, live):
    groups = dims[0]
    lines = cell.shape[0]
    band = up(YP * groups + 2, 16)
    work = 2 * (YP * groups + 2) * 4 * CX * CZ * lines * 128
    vmem = pl.BlockSpec(memory_space=pltpu.VMEM)
    dma = pltpu.SemaphoreType.DMA
    return pl.pallas_call(
        functools.partial(paint_kernel, dims),
        out_shape=jax.ShapeDtypeStruct((groups, ROWS, CZ), jnp.float32),
        in_specs=[pl.BlockSpec(memory_space=pltpu.SMEM)] + [pl.BlockSpec(memory_space=pltpu.HBM)] * 3,
        out_specs=vmem,
        scratch_shapes=[
            pltpu.VMEM((lines, 128), jnp.int32),
            pltpu.VMEM((3, lines, 128), jnp.float32),
            pltpu.VMEM((lines, 128), jnp.float32),
            pltpu.VMEM((6, lines, 128), jnp.float32),
            pltpu.VMEM((6, lines, 128), jnp.float32),
            pltpu.VMEM((14, lines, 128), jnp.float32),
            pltpu.VMEM((6, lines, 128), jnp.float32),
            pltpu.VMEM((lines, 2 * CZ, 128), jnp.bfloat16),
            pltpu.VMEM((lines, 2 * CX, 128), jnp.bfloat16),
            pltpu.VMEM((lines, 2 * BODY + 16, 128), jnp.bfloat16),
            pltpu.VMEM((lines, 4 * band, 128), jnp.bfloat16),
            pltpu.VMEM((lines, 16, 128), jnp.bfloat16),
            pltpu.VMEM((2, 2, band, CX), jnp.float32),
            pltpu.VMEM((2, 2, band, CX), jnp.float32),
            pltpu.VMEM((2, CX + 8, CZ), jnp.float32),
            pltpu.VMEM((2, CX + 8, CZ), jnp.float32),
            pltpu.VMEM((2, 8, CZ), jnp.float32),
            pltpu.VMEM((groups, 8, CZ), jnp.float32),
            pltpu.VMEM((groups, ROWS, CZ), jnp.float32),
            dma((3,)),
            dma((2,)),
            dma((2,)),
            dma((2,)),
            dma((2,)),
            dma((2,)),
            dma((groups,)),
            dma((YP + 1, groups)),
            dma((YP + 1, groups)),
            pltpu.SemaphoreType.REGULAR,
        ],
        cost_estimate=pl.CostEstimate(flops=work, bytes_accessed=24 * lines * 128, transcendentals=0),
        compiler_params=pltpu.CompilerParams(
            collective_id=0, has_side_effects=True, vmem_limit_bytes=32 * 1024 * 1024
        ),
    )(live, *(pltpu.with_memory_space_constraint(value, pltpu.HBM) for value in (cell, offs, mass)))


def wave_kernel(groups, in_ref, table, dens_hbm, spec_hbm, flat, dens_ref, spec_ref, sems):
    length = groups * CX
    row_id = lax.broadcasted_iota(jnp.int32, (CX, CZ), 0)
    lane = lax.broadcasted_iota(jnp.int32, (CX, CZ), 1)
    columns = jnp.concatenate([in_ref[block, BODY:ROWS] for block in range(groups)], axis=0).T
    copies = []
    for block in range(groups):
        before, after = (block - 1) % groups, (block + 1) % groups
        for row in range(YP):
            value = in_ref[block, row * CX : (row + 1) * CX]
            upper = BODY + 2 + row
            value = value + jnp.where(row_id == 0, in_ref[before, upper : upper + 1], 0.0)
            lower = BODY + row
            value = value + jnp.where(row_id == CX - 1, in_ref[after, lower : lower + 1], 0.0)
            ends = [columns[:, 8 * block + 4 + 2 * side + row :][:, :1] for side in range(2)]
            value = value + jnp.where(lane == CZ - 1, ends[0], jnp.where(lane == 0, ends[1], 0.0))
            dens_ref[pl.ds(block * BODY + row, CX, stride=YP), :] = value
            high, low = split(value)
            flat[0, pl.ds(block * CX, CX), pl.ds(row * CZ, CZ)] = high
            flat[1, pl.ds(block * CX, CX), pl.ds(row * CZ, CZ)] = low
        here = pl.ds(block * BODY, BODY)
        copies.append(pltpu.make_async_copy(dens_ref.at[here], dens_hbm.at[here], sems.at[block]))
        copies[-1].start()
    tiles = 4
    tile = length // tiles
    for turn in range(tiles):
        rows = pl.ds(turn * tile, tile)
        both = jnp.dot(table[0, rows, :], flat[0], preferred_element_type=jnp.float32)
        both += jnp.dot(table[1, rows, :], flat[0], preferred_element_type=jnp.float32)
        both += jnp.dot(table[0, rows, :], flat[1], preferred_element_type=jnp.float32)
        for row in range(YP):
            spec_ref[pl.ds(turn * tile * YP + row, tile, stride=YP), :] = both[:, row * CZ : (row + 1) * CZ]
        here = pl.ds(turn * tile * YP, tile * YP)
        copies.append(pltpu.make_async_copy(spec_ref.at[here], spec_hbm.at[here], sems.at[groups + turn]))
        copies[-1].start()
    for copy in copies:
        copy.wait()


def waves(groups, pencils):
    length = groups * CX
    half = length // 2
    angle = (np.arange(half)[:, None] * np.arange(length)[None, :] % length) * (2.0 * np.pi / length)
    table = np.concatenate([np.cos(angle), -np.sin(angle)]) / np.sqrt(length)
    fhi = table.astype(jnp.bfloat16)
    flo = (table - fhi.astype(np.float64)).astype(jnp.bfloat16)
    vmem = pl.BlockSpec(memory_space=pltpu.VMEM)
    return pl.pallas_call(
        functools.partial(wave_kernel, groups),
        out_shape=[
            jax.ShapeDtypeStruct((length * YP, CZ), jnp.float32),
            jax.ShapeDtypeStruct((2 * half * YP, CZ), jnp.float32),
        ],
        in_specs=[vmem] * 2,
        out_specs=[pl.BlockSpec(memory_space=pltpu.HBM)] * 2,
        scratch_shapes=[
            pltpu.VMEM((2, length, YP * CZ), jnp.bfloat16),
            pltpu.VMEM((length * YP, CZ), jnp.float32),
            pltpu.VMEM((2 * half * YP, CZ), jnp.float32),
            pltpu.SemaphoreType.DMA((groups + 4,)),
        ],
        compiler_params=pltpu.CompilerParams(vmem_limit_bytes=24 * 1024 * 1024),
    )(pencils, jnp.asarray(np.stack([fhi, flo])))


def body(dims, cell_index, offsets, mass, counts):
    length = dims[0] * CX
    pencils = paint(
        dims, cell_index.reshape(-1, 128), offsets.reshape(3, -1, 128), mass.reshape(-1, 128), counts.reshape(1)
    )
    density, spectrum = waves(dims[0], pencils)
    return (density.reshape(length, 1, YP, CZ), spectrum.reshape(2, length // 2, 1, YP, CZ))


def solution(mesh):
    dims = tuple(mesh.shape[axis] for axis in ("gx", "gy", "gz"))
    placed = (
        P("gx", "gy", "gz", None),
        P("gx", "gy", "gz", None, None),
        P("gx", "gy", "gz", None),
        P("gx", "gy", "gz"),
    )
    return jax.shard_map(
        functools.partial(body, dims),
        mesh=mesh,
        in_specs=placed,
        out_specs=(P(None, "gx", "gy", "gz"), P(None, None, "gx", "gy", "gz")),
        check_vma=False,
    )
```

```python
import functools
import math

import jax
import jax.numpy as jnp
import numpy as np
from jax import lax
from jax.experimental import pallas as pl
from jax.experimental.pallas import tpu as pltpu
from jax.sharding import PartitionSpec as P

MESH = pl.DeviceIdType.MESH
CX = 128
YP = 2
CZ = 128


def up(n, m):
    return -(-n // m) * m


def split(value):
    high = value.astype(jnp.bfloat16)
    low = (value - high.astype(jnp.float32)).astype(jnp.bfloat16)
    return high, low


def nt_dot(lhs, rhs):
    return lax.dot_general(lhs, rhs, (((1,), (1,)), ((), ())), preferred_element_type=jnp.float32)


def gather(full, rows):
    return (full[:rows, :128] + full[rows:, :128]) + (full[:rows, 128:] + full[rows:, 128:])


BODY = YP * CX
ROWS = BODY + 8


def parts(value):
    high = value.astype(jnp.bfloat16).astype(jnp.float32)
    return high, value - high


def paint_kernel(dims, live_ref, cell_hbm, off_hbm, mass_hbm, out_ref, cell_ref, off_ref, mass_ref, rows_x, rows_z, weigh, spot, zrhs, xrhs, lhs, glhs, crhs, fold_z, zin, yout, yin, fout, fin, pen, load, z_send, z_recv, y_send, y_recv, f_send, f_recv, x_send, x_recv, opened):
    groups, count_y, count_z = dims
    padded_y = YP * groups + 2
    band = up(padded_y, 16)
    loads = [
        pltpu.make_async_copy(source, target, load.at[index])
        for index, (source, target) in enumerate(((cell_hbm, cell_ref), (off_hbm, off_ref), (mass_hbm, mass_ref)))
    ]
    for copy in loads:
        copy.start()
    stride_y = CZ + 2
    stride_x = padded_y * stride_y
    lines = cell_ref.shape[0]
    span = min(16, lines)
    pieces = lines // span
    gx, gy, gz = lax.axis_index("gx"), lax.axis_index("gy"), lax.axis_index("gz")
    y_next = (lax.rem(gy + count_y - 1, count_y), lax.rem(gy + 1, count_y))
    z_next = (lax.rem(gz + count_z - 1, count_z), lax.rem(gz + 1, count_z))
    barrier = pltpu.get_barrier_semaphore()
    for other in z_next:
        pl.semaphore_signal(barrier, inc=1, device_id={"gz": other}, device_id_type=MESH)
    for other in y_next:
        pl.semaphore_signal(barrier, inc=1, device_id={"gy": other}, device_id_type=MESH)
    for step in range(1, groups):
        pl.semaphore_signal(barrier, inc=1, device_id={"gx": lax.rem(gx + step, groups)}, device_id_type=MESH)
    for copy in loads:
        copy.wait()
    live = live_ref[0]
    slot = lax.broadcasted_iota(jnp.int32, (lines, 128), 0) * 128 + lax.broadcasted_iota(jnp.int32, (lines, 128), 1)
    loaded = jnp.where(slot < live, mass_ref[...], 0.0)
    cell = cell_ref[...].astype(jnp.float32)
    x0 = jnp.floor((cell + 0.5) * (1.0 / stride_x))
    rest = cell - x0 * stride_x
    y0 = jnp.floor((rest + 0.5) * (1.0 / stride_y))
    z0 = rest - y0 * stride_y
    dx, dy, dz = off_ref[0], off_ref[1], off_ref[2]
    x1 = x0 + jnp.where(dx >= 0.0, 1.0, -1.0)
    y1 = y0 + jnp.where(dy >= 0.0, 1.0, -1.0)
    z1 = z0 + jnp.where(dz >= 0.0, 1.0, -1.0)
    fx, fy, fz = jnp.abs(dx), jnp.abs(dy), jnp.abs(dz)
    ex, ey, ez = 1.0 - fx, 1.0 - fy, 1.0 - fz
    my0, my1 = ey * loaded, fy * loaded
    spot[0], spot[1], spot[2], spot[3] = y0, y1, my0, my1
    spot[4], spot[5] = ex, fx
    for index, value in enumerate((x0, x1) + parts(ex) + parts(fx)):
        rows_x[index] = value
    for index, value in enumerate((z0, z1) + parts(ez) + parts(fz)):
        rows_z[index] = value
    far_x, far_z = CX + 1.0, CZ + 1.0
    gz_y = jnp.where(z1 == 0.0, 0.0, jnp.where(z1 == far_z, float(band), -1.0 - band))
    ghost_rows = (gz_y + y0, gz_y + y1) + parts(fz * my0) + parts(fz * my1)
    for index, value in enumerate(ghost_rows):
        weigh[8 + index] = value

    def row(ref, index, line):
        value = ref[index, pl.ds(line, 1), :]
        return jnp.broadcast_to(value, (16, 128)).astype(jnp.bfloat16)[None]

    zero = jnp.zeros((1, 16, 128), jnp.bfloat16)
    count = lax.broadcasted_iota(jnp.int32, (CX // 16, 16, 128), 0) * 16 + lax.broadcasted_iota(jnp.int32, (CX // 16, 16, 128), 1)
    core = (count + 1).astype(jnp.float32).astype(jnp.bfloat16)
    banded = count.astype(jnp.float32).astype(jnp.bfloat16)[: 2 * band // 16]
    sides = lax.broadcasted_iota(jnp.int32, (1, 16, 128), 1)
    edge_row = jnp.where(sides < 4 * YP, jnp.where(lax.rem(sides, 2) == 0, 0.0, far_x), -9.0).astype(jnp.bfloat16)
    level = sides.astype(jnp.float32).astype(jnp.bfloat16)
    side_row = jnp.where(lax.rem(sides, 2) == 0, 0.0, far_x).astype(jnp.bfloat16)
    top = jnp.where(sides < 2, 1.0, 0.0).astype(jnp.bfloat16)

    def hot(ref, line, at=0, rows=core):
        first, second = rows == row(ref, at, line), rows == row(ref, at + 1, line)
        high = jnp.where(first, row(ref, at + 2, line), jnp.where(second, row(ref, at + 4, line), zero))
        low = jnp.where(first, row(ref, at + 3, line), jnp.where(second, row(ref, at + 5, line), zero))
        return high.reshape(-1, 128), low.reshape(-1, 128)

    def across(piece, store):
        for line in range(span):
            store(piece * span + line)

    def build_ghost(line):
        high, low = hot(weigh, line, 8, banded)
        glhs[line, pl.ds(0, 2 * band)] = high
        glhs[line, pl.ds(2 * band, 2 * band)] = low

    def build_x(line):
        high, low = hot(rows_x, line)
        xrhs[line, pl.ds(0, CX)] = high
        xrhs[line, pl.ds(CX, CX)] = low
        match = side_row == row(rows_x, 1, line)
        pick = jnp.where(top > zero, row(rows_x, 4, line), row(rows_x, 5, line))
        crhs[line] = jnp.where(match, pick, zero).reshape(16, 128)

    def build_z(line):
        high, low = hot(rows_z, line)
        zrhs[line, pl.ds(0, CZ)] = high
        zrhs[line, pl.ds(CZ, CZ)] = low

    def wide(ref, start, width):
        return jnp.concatenate([ref[start + line] for line in range(width)], axis=1)

    def total(terms):
        sums = None
        for term in terms:
            sums = term if sums is None else sums + term
        return sums

    def paint_rows(first, second):
        for index, y in enumerate((first, second)):
            wy = jnp.where(spot[0] == y, spot[2], jnp.where(spot[1] == y, spot[3], 0.0))
            for place, value in enumerate(parts(spot[4] * wy) + parts(spot[5] * wy)):
                weigh[4 * index + place] = value

        def build(line):
            near, far = core == row(rows_x, 0, line), core == row(rows_x, 1, line)
            for index in range(2):
                for part in range(2):
                    value = jnp.where(near, row(weigh, 4 * index + part, line), jnp.where(far, row(weigh, 4 * index + 2 + part, line), zero))
                    lhs[line, pl.ds((2 * index + part) * CX, CX)] = value.reshape(CX, 128)
            pick = zero
            for index in reversed(range(4)):
                pick = jnp.where(level < jnp.bfloat16(2 * index + 2), row(weigh, 4 * (index // 2) + 2 + index % 2, line), pick)
            pick = jnp.where(edge_row == row(rows_x, 1, line), pick, zero)
            lhs[line, pl.ds(2 * BODY, 16)] = pick.reshape(16, 128)

        terms = []
        for piece in range(pieces):
            across(piece, build)
            terms.append(nt_dot(wide(lhs, piece * span, span), wide(zrhs, piece * span, span)))
        sums = total(terms)
        edges = sums[2 * BODY :, :128] + sums[2 * BODY :, 128:]
        return gather(sums[: 2 * CX], CX), gather(sums[2 * CX : 2 * BODY], CX), edges

    edge_lane = lax.broadcasted_iota(jnp.int32, (1, CZ), 1)
    half = groups // 2
    upper = gx // half

    def pencil_of(turn):
        mine = upper * (groups - 1) + (1 - 2 * upper) * gx
        near_by = turn - (groups - half)
        near_by = near_by + jnp.where(near_by >= mine, 1, 0)
        place = jnp.where(turn < groups - half, half + turn, jnp.where(turn == groups - 1, mine, near_by))
        return upper * (groups - 1) + (1 - 2 * upper) * place

    def part_copy(target, part):
        size = CX if part is not YP else 8
        here = pl.ds(pl.multiple_of(part * CX, 8), size)
        return pltpu.make_async_remote_copy(
            src_ref=pen.at[target, here],
            dst_ref=out_ref.at[gx, here],
            send_sem=x_send.at[part, target],
            recv_sem=x_recv.at[part, gx],
            device_id={"gx": target},
            device_id_type=MESH,
        )

    y_copies = [
        pltpu.make_async_remote_copy(
            src_ref=yout.at[side],
            dst_ref=yin.at[side],
            send_sem=y_send.at[side],
            recv_sem=y_recv.at[side],
            device_id={"gy": y_next[side]},
            device_id_type=MESH,
        )
        for side in range(2)
    ]
    far_copies = [
        pltpu.make_async_remote_copy(
            src_ref=fout.at[side],
            dst_ref=fin.at[gx],
            send_sem=f_send.at[side],
            recv_sem=f_recv.at[gx],
            device_id={"gx": jnp.int32((groups - 1) * (1 - side)), "gy": y_next[side]},
            device_id_type=MESH,
        )
        for side in range(2)
    ]

    def put(target, main, edge, pitch, rows, at):
        edges = rows[YP]
        target[pl.ds(main, CX)] = rows[at]
        for side in range(2):
            low = 4 * at + side
            target[pl.ds(edge + pitch * side, 1)] = edges[low : low + 1] + edges[low + 2 : low + 3]

    def put_pen(target, place, rows, at):
        put(pen.at[target], pl.multiple_of(place * CX, 8), BODY + place, 2, rows, at)

    def corners(index):
        ends = [zin[side, 1, pl.ds(index, 1)] for side in range(2)]
        for side in range(2):
            extra = jnp.where(edge_lane == CZ - 1, ends[0][:, side : side + 1], 0.0)
            yield extra + jnp.where(edge_lane == 0, ends[1][:, side : side + 1], 0.0)

    def finish(target, place):
        index = 1 + target * YP + place
        for side, extra in enumerate(corners(index)):
            pen[target, pl.ds(BODY + 2 * side + place, 1)] += extra
            pen[target, pl.ds(BODY + 4 + 2 * side + place, 1)] = zin[side, 0, pl.ds(index, 1)]

    def send_corners():
        for side, index in enumerate((0, padded_y - 1)):
            for kind, extra in enumerate(corners(index)):
                fout[side, pl.ds(kind, 1)] = extra
                fout[side, pl.ds(2 + kind, 1)] = zin[kind, 0, pl.ds(index, 1)]
            far_copies[side].start()

    def add_first():
        pen[0, pl.ds(0, CX)] += yin[1, pl.ds(0, CX)]
        for side in range(2):
            pen[0, pl.ds(BODY + 2 * side, 1)] += yin[1, pl.ds(CX + side, 1)]

    def add_last():
        pen[groups - 1, pl.ds((YP - 1) * CX, CX)] += yin[0, pl.ds(0, CX)]
        for side in range(2):
            pen[groups - 1, pl.ds(BODY + 2 * side + YP - 1, 1)] += yin[0, pl.ds(CX + side, 1)]

    late = groups - half

    def line_of(target, place):
        return 1 + target * YP + place

    def as_float(indices):
        return [index.astype(jnp.float32) for index in indices]

    def build_all(piece, carry):
        across(piece, build_z)
        return carry

    lax.fori_loop(0, pieces, build_all, 0)
    leader = pencil_of(jnp.int32(0))
    rows = paint_rows(*as_float([line_of(leader, place) for place in range(YP)]))
    for place in range(YP):
        put_pen(leader, place, rows, place)
    pl.semaphore_wait(barrier, groups + 3)

    @pl.when(jnp.logical_or(gx == 0, gx == groups - 1))
    def _():
        for step in range(1, groups):
            pl.semaphore_signal(
                opened, inc=1, device_id={"gx": lax.rem(gx + step, groups)}, device_id_type=MESH
            )

    for part in range(YP):
        part_copy(leader, part).start()

    z_copies = [
        pltpu.make_async_remote_copy(
            src_ref=fold_z.at[side],
            dst_ref=zin.at[side],
            send_sem=z_send.at[side],
            recv_sem=z_recv.at[side],
            device_id={"gz": z_next[side]},
            device_id_type=MESH,
        )
        for side in range(2)
    ]
    def send_ghosts():
        step = span // 2
        terms = ([], [])
        for piece in range(pieces):
            across(piece, build_x)
            across(piece, build_ghost)
            for side in range(2):
                start = piece * span + side * step
                terms[side].append(nt_dot(wide(glhs, start, step), wide(xrhs, start, step)))
        sums = [total(terms[side]) for side in range(2)]
        ends = total(nt_dot(wide(glhs, piece * span, span), wide(crhs, piece * span, span)) for piece in range(pieces))
        sums = gather(sums[0] + sums[1], 2 * band)
        ends = ends[: 2 * band] + ends[2 * band :]
        ends = ends[:, :2] + ends[:, 2:4]
        for side in range(2):
            here = slice(side * band, side * band + band)
            fold_z[side, 0] = sums[here]
            fold_z[side, 1] = jnp.zeros((band, CX), jnp.float32)
            fold_z[side, 1, :, pl.ds(0, 2)] = ends[here]
        for copy in z_copies:
            copy.start()

    yout[:, pl.ds(CX, 8)] = jnp.zeros((2, 8, CZ), jnp.float32)
    fout[...] = jnp.zeros_like(fout)
    held, close = pencil_of(jnp.int32(late - 1)), pencil_of(jnp.int32(late))

    def visit(turn, carry):
        whole = pencil_of(turn - 1)
        opening, closing, joining = turn == 1, turn == late, turn == late + 1
        first = jnp.where(joining, line_of(held, 1 - upper), line_of(whole, 0))
        second = jnp.where(joining, line_of(close, upper), line_of(whole, 1))
        first = jnp.where(opening, upper * (padded_y - 1), jnp.where(closing, line_of(close, 1 - upper), first))
        second = jnp.where(opening, line_of(held, upper), jnp.where(closing, (1 - upper) * (padded_y - 1), second))
        rows = paint_rows(*as_float((first, second)))

        @pl.when(opening)
        def _():
            put(yout.at[upper], 0, CX, 1, rows, 0)
            for side in range(2):
                pl.when(upper == side)(y_copies[side].start)
            put_pen(held, upper, rows, 1)
            part_copy(held, upper).start()

        @pl.when(closing)
        def _():
            put_pen(close, 1 - upper, rows, 0)
            part_copy(close, 1 - upper).start()
            put(yout.at[1 - upper], 0, CX, 1, rows, 1)
            for side in range(2):
                pl.when(upper == 1 - side)(y_copies[side].start)
            send_ghosts()

        @pl.when(joining)
        def _():
            put_pen(held, 1 - upper, rows, 0)
            for side in range(2):

                @pl.when(upper == side)
                def _():
                    y_copies[side].wait()
                    (add_first if side else add_last)()

            part_copy(held, 1 - upper).start()
            put_pen(close, upper, rows, 1)
            for copy in z_copies:
                copy.wait()
            pl.semaphore_wait(opened, jnp.where(jnp.logical_or(gx == 0, gx == groups - 1), 1, 2))
            send_corners()
            for order in range(late):
                target = pencil_of(jnp.int32(order))
                for place in range(YP):
                    finish(target, place)
                part_copy(target, YP).start()
            for place in range(YP):
                finish(close, place)
            for side in range(2):

                @pl.when(upper == 1 - side)
                def _():
                    y_copies[side].wait()
                    pl.when(gx != (groups - 1) * (1 - side))(add_first if side else add_last)

            part_copy(close, upper).start()
            part_copy(close, YP).start()

        @pl.when(jnp.logical_not(jnp.logical_or(opening, jnp.logical_or(closing, joining))))
        def _():
            for place in range(YP):
                put_pen(whole, place, rows, place)

            @pl.when(turn < late)
            def _():
                for place in range(YP):
                    part_copy(whole, place).start()

            @pl.when(turn > late + 1)
            def _():
                for place in range(YP):
                    finish(whole, place)

                @pl.when(turn < groups)
                def _():
                    for part in range(YP + 1):
                        part_copy(whole, part).start()

        return carry

    lax.fori_loop(1, groups + 1, visit, 0)
    pl.when(gx == 0)(add_first)
    pl.when(gx == groups - 1)(add_last)
    out_ref[gx] = pen[gx]
    for step in range(1, groups):
        source = lax.rem(gx + step, groups)
        for part in range(YP + 1):
            here = pl.ds(part * CX, CX if part < YP else 8)
            part_copy(source, part).wait_send()
            pltpu.make_async_remote_copy(
                src_ref=pen.at[source, here],
                dst_ref=out_ref.at[source, here],
                send_sem=x_send.at[part, source],
                recv_sem=x_recv.at[part, source],
                device_id={"gx": source},
                device_id_type=MESH,
            ).wait_recv()
    for side in range(2):
        far_copies[side].wait_send()
    for side, owner in enumerate((groups - 1, 0)):

        @pl.when(gx == owner)
        def _():
            for source in range(groups):
                pltpu.make_async_remote_copy(
                    src_ref=fout.at[side],
                    dst_ref=fin.at[source],
                    send_sem=f_send.at[side],
                    recv_sem=f_recv.at[source],
                    device_id={"gx": jnp.int32(source), "gy": y_next[side]},
                    device_id_type=MESH,
                ).wait_recv()
                for kind in range(4):
                    at = pl.ds(BODY + 2 * kind + (YP - 1) * (1 - side), 1)
                    out_ref[source, at] += fin[source, pl.ds(kind, 1)]


def paint(dims, cell, offs, mass, live):
    groups = dims[0]
    lines = cell.shape[0]
    band = up(YP * groups + 2, 16)
    work = 2 * (YP * groups + 2) * 4 * CX * CZ * lines * 128
    vmem = pl.BlockSpec(memory_space=pltpu.VMEM)
    dma = pltpu.SemaphoreType.DMA
    return pl.pallas_call(
        functools.partial(paint_kernel, dims),
        out_shape=jax.ShapeDtypeStruct((groups, ROWS, CZ), jnp.float32),
        in_specs=[pl.BlockSpec(memory_space=pltpu.SMEM)] + [pl.BlockSpec(memory_space=pltpu.HBM)] * 3,
        out_specs=vmem,
        scratch_shapes=[
            pltpu.VMEM((lines, 128), jnp.int32),
            pltpu.VMEM((3, lines, 128), jnp.float32),
            pltpu.VMEM((lines, 128), jnp.float32),
            pltpu.VMEM((6, lines, 128), jnp.float32),
            pltpu.VMEM((6, lines, 128), jnp.float32),
            pltpu.VMEM((14, lines, 128), jnp.float32),
            pltpu.VMEM((6, lines, 128), jnp.float32),
            pltpu.VMEM((lines, 2 * CZ, 128), jnp.bfloat16),
            pltpu.VMEM((lines, 2 * CX, 128), jnp.bfloat16),
            pltpu.VMEM((lines, 2 * BODY + 16, 128), jnp.bfloat16),
            pltpu.VMEM((lines, 4 * band, 128), jnp.bfloat16),
            pltpu.VMEM((lines, 16, 128), jnp.bfloat16),
            pltpu.VMEM((2, 2, band, CX), jnp.float32),
            pltpu.VMEM((2, 2, band, CX), jnp.float32),
            pltpu.VMEM((2, CX + 8, CZ), jnp.float32),
            pltpu.VMEM((2, CX + 8, CZ), jnp.float32),
            pltpu.VMEM((2, 8, CZ), jnp.float32),
            pltpu.VMEM((groups, 8, CZ), jnp.float32),
            pltpu.VMEM((groups, ROWS, CZ), jnp.float32),
            dma((3,)),
            dma((2,)),
            dma((2,)),
            dma((2,)),
            dma((2,)),
            dma((2,)),
            dma((groups,)),
            dma((YP + 1, groups)),
            dma((YP + 1, groups)),
            pltpu.SemaphoreType.REGULAR,
        ],
        cost_estimate=pl.CostEstimate(flops=work, bytes_accessed=24 * lines * 128, transcendentals=0),
        compiler_params=pltpu.CompilerParams(
            collective_id=0, has_side_effects=True, vmem_limit_bytes=32 * 1024 * 1024
        ),
    )(live, *(pltpu.with_memory_space_constraint(value, pltpu.HBM) for value in (cell, offs, mass)))


def wave_kernel(groups, in_ref, table, dens_hbm, spec_hbm, flat, dens_ref, spec_ref, sems):
    length = groups * CX
    row_id = lax.broadcasted_iota(jnp.int32, (CX, CZ), 0)
    lane = lax.broadcasted_iota(jnp.int32, (CX, CZ), 1)
    columns = jnp.concatenate([in_ref[block, BODY:ROWS] for block in range(groups)], axis=0).T
    copies = []
    for block in range(groups):
        before, after = (block - 1) % groups, (block + 1) % groups
        for row in range(YP):
            value = in_ref[block, row * CX : (row + 1) * CX]
            upper = BODY + 2 + row
            value = value + jnp.where(row_id == 0, in_ref[before, upper : upper + 1], 0.0)
            lower = BODY + row
            value = value + jnp.where(row_id == CX - 1, in_ref[after, lower : lower + 1], 0.0)
            ends = [columns[:, 8 * block + 4 + 2 * side + row :][:, :1] for side in range(2)]
            value = value + jnp.where(lane == CZ - 1, ends[0], jnp.where(lane == 0, ends[1], 0.0))
            dens_ref[pl.ds(block * BODY + row, CX, stride=YP), :] = value
            high, low = split(value)
            flat[0, pl.ds(block * CX, CX), pl.ds(row * CZ, CZ)] = high
            flat[1, pl.ds(block * CX, CX), pl.ds(row * CZ, CZ)] = low
        here = pl.ds(block * BODY, BODY)
        copies.append(pltpu.make_async_copy(dens_ref.at[here], dens_hbm.at[here], sems.at[block]))
        copies[-1].start()
    tiles = 4
    tile = length // tiles
    for turn in range(tiles):
        rows = pl.ds(turn * tile, tile)
        both = jnp.dot(table[0, rows, :], flat[0], preferred_element_type=jnp.float32)
        both += jnp.dot(table[1, rows, :], flat[0], preferred_element_type=jnp.float32)
        both += jnp.dot(table[0, rows, :], flat[1], preferred_element_type=jnp.float32)
        for row in range(YP):
            spec_ref[pl.ds(turn * tile * YP + row, tile, stride=YP), :] = both[:, row * CZ : (row + 1) * CZ]
        here = pl.ds(turn * tile * YP, tile * YP)
        copies.append(pltpu.make_async_copy(spec_ref.at[here], spec_hbm.at[here], sems.at[groups + turn]))
        copies[-1].start()
    for copy in copies:
        copy.wait()


def waves(groups, pencils):
    length = groups * CX
    half = length // 2
    angle = (np.arange(half)[:, None] * np.arange(length)[None, :] % length) * (2.0 * np.pi / length)
    table = np.concatenate([np.cos(angle), -np.sin(angle)]) / np.sqrt(length)
    fhi = table.astype(jnp.bfloat16)
    flo = (table - fhi.astype(np.float64)).astype(jnp.bfloat16)
    vmem = pl.BlockSpec(memory_space=pltpu.VMEM)
    return pl.pallas_call(
        functools.partial(wave_kernel, groups),
        out_shape=[
            jax.ShapeDtypeStruct((length * YP, CZ), jnp.float32),
            jax.ShapeDtypeStruct((2 * half * YP, CZ), jnp.float32),
        ],
        in_specs=[vmem] * 2,
        out_specs=[pl.BlockSpec(memory_space=pltpu.HBM)] * 2,
        scratch_shapes=[
            pltpu.VMEM((2, length, YP * CZ), jnp.bfloat16),
            pltpu.VMEM((length * YP, CZ), jnp.float32),
            pltpu.VMEM((2 * half * YP, CZ), jnp.float32),
            pltpu.SemaphoreType.DMA((groups + 4,)),
        ],
        compiler_params=pltpu.CompilerParams(vmem_limit_bytes=24 * 1024 * 1024),
    )(pencils, jnp.asarray(np.stack([fhi, flo])))


def body(dims, cell_index, offsets, mass, counts):
    length = dims[0] * CX
    pencils = paint(
        dims, cell_index.reshape(-1, 128), offsets.reshape(3, -1, 128), mass.reshape(-1, 128), counts.reshape(1)
    )
    density, spectrum = waves(dims[0], pencils)
    return (density.reshape(length, 1, YP, CZ), spectrum.reshape(2, length // 2, 1, YP, CZ))


def solution(mesh):
    dims = tuple(mesh.shape[axis] for axis in ("gx", "gy", "gz"))
    placed = (
        P("gx", "gy", "gz", None),
        P("gx", "gy", "gz", None, None),
        P("gx", "gy", "gz", None),
        P("gx", "gy", "gz"),
    )
    return jax.shard_map(
        functools.partial(body, dims),
        mesh=mesh,
        in_specs=placed,
        out_specs=(P(None, "gx", "gy", "gz"), P(None, None, "gx", "gy", "gz")),
        check_vma=False,
    )
```
